32 devices in a mesh: fourier: 2 (over x), ex: 4 (over z), ey: 4 (over y, core).
Axes of the slice: x: 2, y: 2, z: 4, core: 2. Of those that a mesh axis runs over, the one named last changes fastest.
Arguments:
- forcing: float32 [128, 81, 2048], P('fourier', None, ('ex', 'ey')), may hold values from -6 to 6
- element_coef: float32 [2048], P(('ex', 'ey')), may hold values from 0.5 to 2
- schur: float32 [128, 32, 32], P('fourier'), may hold values from -12 to 20, as said below
- couple: float32 [128, 32, 49], P('fourier'), may hold values from -0.875 to 0.875
- inner_inv: float32 [128, 49, 49], P('fourier'), may hold values from -3 to 4.5, as said below
- element_cell: int32 [2048], P(('ex', 'ey')), may hold values from 0 to 127, as said below
Outputs:
- velocity: float32 [128, 81, 2048], P('fourier', None, ('ex', 'ey'))
The draws below stay inside these ranges and needn't reach their ends.
Inputs may be any that keep to these rules, and one draw needn't show every extreme that they name: `element_cell`: each aligned block of 128 entries is a permutation of 0 to 127. `schur`: each matrix is symmetric positive definite. `inner_inv`: each matrix is symmetric positive definite.
All inputs are finite; a program needn't handle non-finite values.
Results may differ from the reference program's by a relative error of at most 0.0001.
Values sent between devices are 32-bit elements; how exact they have to be, the bound alone decides.
A program may use at most 128 MiB of HBM per device.

```python
import math
import jax
import jax.numpy as jnp
import numpy as np
from jax import lax

P_SIZE = 8
NZ = 128
ITERS = 3
ELX = 8
ELY = 16
NODES = 81
NB = 32
NI = 49
EL_DEV = 128
ELEMENTS = 2048
NXE = 32
NYE = 64
N_EY = 4


def draw_schur(key, part):
    first, second = jax.random.split(jax.random.fold_in(key, 11), 2)
    width = 4 * P_SIZE
    factor = jax.random.uniform(first, (NZ, width, width), jnp.float32, -math.sqrt(3.0), math.sqrt(3.0))
    shift = jnp.exp(jax.random.uniform(second, (NZ, 1, 1), jnp.float32, math.log(0.5), math.log(2.0)))
    matrix = jnp.einsum('mab,mcb->mac', factor, factor) / width + shift * jnp.eye(width, dtype=jnp.float32)
    return matrix


def draw_inner_inv(key, part):
    first, second = jax.random.split(jax.random.fold_in(key, 23), 2)
    width = (P_SIZE - 1) ** 2
    factor = jax.random.uniform(first, (NZ, width, width), jnp.float32, -math.sqrt(3.0), math.sqrt(3.0))
    shift = jax.random.uniform(second, (NZ, 1, 1), jnp.float32, 0.5, 1.5)
    return jnp.einsum('mab,mcb->mac', factor, factor) / width + shift * jnp.eye(width, dtype=jnp.float32)


def draw_element_cell(key, part):
    keys = jax.random.split(jax.random.fold_in(key, 37), ELEMENTS // EL_DEV)
    orders = jax.vmap(lambda single: jax.random.permutation(single, EL_DEV))(keys)
    return orders.reshape(-1).astype(jnp.int32)


def level_of(stream_key, extent, pieces, least, high):
    def one(position, shards_of):
        heights = jax.random.uniform(jax.random.fold_in(jax.random.fold_in(stream_key, 6), position), (shards_of,), jnp.float32, least / len(pieces), high / len(pieces))
        return jnp.repeat(jnp.exp(heights), extent[position] // shards_of).reshape((-1,) + (1,) * (len(extent) - position - 1))

    factor_of = one(*pieces[0])
    for cut in pieces[1:]:
        factor_of = factor_of * one(*cut)
    return factor_of


def normal_values(own_key, dims, scale, limit, pieces=(), kind=jnp.bfloat16):
    drawn = jax.random.normal(own_key, dims, jnp.float32) * scale
    if len(pieces) > 0:
        drawn = level_of(own_key, dims, pieces, -0.22, 0.18) * drawn
    return jnp.clip(drawn, min=-limit, max=limit).astype(kind)


def setup_inputs(seed: int = 0) -> dict:
    arg_keys = jax.random.split(jax.random.key(seed), 7)
    forcing = normal_values(arg_keys[0], (NZ, NODES, ELEMENTS), 1.0, 6.0, ((0, 2), (2, 16)), jnp.float32)
    element_coef = jnp.clip(jnp.exp(math.log(2.0) - 1.3862944 * jax.random.uniform(arg_keys[1], (ELEMENTS,), jnp.float32) ** level_of(arg_keys[1], (ELEMENTS,), ((0, 16),), -0.2, 0.2)), 0.5, 2.0)
    schur = draw_schur(jax.random.fold_in(arg_keys[6], 71), 0)
    couple = normal_values(arg_keys[3], (NZ, NB, NI), NI ** -0.5, 0.875, ((0, 2),), jnp.float32)
    inner_inv = draw_inner_inv(jax.random.fold_in(arg_keys[6], 71), 0)
    element_cell = draw_element_cell(jax.random.fold_in(arg_keys[6], 71), 0)
    return {"forcing": forcing, "element_coef": element_coef, "schur": schur, "couple": couple, "inner_inv": inner_inv, "element_cell": element_cell}


def dft_rows(length):
    row_index = jnp.arange(length)[:, None]
    plane_pos = jnp.arange(length, dtype=jnp.float32)[None, :]
    waves = ((row_index + 1) // 2).astype(jnp.float32)
    angles = 2.0 * math.pi * waves * plane_pos / length
    factor = math.sqrt(2.0 / length)
    result = jnp.where(row_index % 2 == 1, factor * jnp.cos(angles), factor * jnp.sin(angles))
    result = jnp.where(row_index == 0, 1.0 / math.sqrt(length), result)
    result = jnp.where(row_index == length - 1, jnp.cos(math.pi * plane_pos) / math.sqrt(length), result)
    return result.astype(jnp.float32)

def node_masks(row_ids, col_ids, rows_total, cols_total):
    slots = np.arange(4 * P_SIZE)
    on_left = jnp.asarray((slots == 0) | (slots >= 3 * P_SIZE))[:, None, None]
    on_right = jnp.asarray((slots >= P_SIZE) & (slots <= 2 * P_SIZE))[:, None, None]
    on_bottom = jnp.asarray(slots <= P_SIZE)[:, None, None]
    on_top = jnp.asarray((slots >= 2 * P_SIZE) & (slots <= 3 * P_SIZE))[:, None, None]
    dropped = on_left & (row_ids == 0)[None, :, None] | on_right & (row_ids == rows_total - 1)[None, :, None]
    dropped = dropped | on_bottom & (col_ids == 0)[None, None, :] | on_top & (col_ids == cols_total - 1)[None, None, :]
    keep = jnp.where(dropped, 0.0, 1.0).astype(jnp.float32)
    corner_weight = jnp.asarray(np.where(slots % P_SIZE == 0, 0.25, 0.5)).astype(jnp.float32)
    return (keep, keep * corner_weight[:, None, None])

def side_lines(values):
    return (jnp.concatenate([values[:, 0:1], values[:, 4 * P_SIZE - 1:3 * P_SIZE - 1:-1]], 1), values[:, P_SIZE:2 * P_SIZE + 1])

def add_sides(values, left_next, right_prev):
    blank = jnp.zeros((values.shape[0], P_SIZE - 1) + values.shape[2:], values.dtype)
    return values + jnp.concatenate([right_prev[:, 0:1], blank, left_next, blank, right_prev[:, P_SIZE:0:-1]], 1)

def end_lines(values):
    return (values[:, 0:P_SIZE + 1], values[:, 3 * P_SIZE:2 * P_SIZE - 1:-1])

def add_ends(values, bottom_next, top_prev):
    blank = jnp.zeros((values.shape[0], P_SIZE - 1) + values.shape[2:], values.dtype)
    return values + jnp.concatenate([top_prev, blank, bottom_next[:, ::-1], blank], 1)

def assemble(values):
    left_line, right_line = side_lines(values)
    left_next = jnp.pad(left_line[:, :, 1:], ((0, 0), (0, 0), (0, 1), (0, 0)))
    right_prev = jnp.pad(right_line[:, :, :-1], ((0, 0), (0, 0), (1, 0), (0, 0)))
    values = add_sides(values, left_next, right_prev)
    bottom_line, top_line = end_lines(values)
    bottom_next = jnp.pad(bottom_line[:, :, :, 1:], ((0, 0), (0, 0), (0, 0), (0, 1)))
    top_prev = jnp.pad(top_line[:, :, :, :-1], ((0, 0), (0, 0), (0, 0), (1, 0)))
    return add_ends(values, bottom_next, top_prev)

def reference(forcing, element_coef, schur, couple, inner_inv, element_cell):
    highest = lax.Precision.HIGHEST
    dft_table = dft_rows(NZ)
    spectral = jnp.einsum('jz,zne->jne', dft_table, forcing, precision=highest)
    block_ids = jnp.arange(ELEMENTS, dtype=jnp.int32) // EL_DEV
    grid_row = block_ids // N_EY * ELX + element_cell // ELY
    grid_col = block_ids % N_EY * ELY + element_cell % ELY
    location = (grid_row * NYE + grid_col).astype(jnp.int32)
    ordering = jnp.zeros((ELEMENTS,), jnp.int32).at[location].set(jnp.arange(ELEMENTS, dtype=jnp.int32))
    gridded = jnp.take(spectral, ordering, axis=2).reshape(NZ, NODES, NXE, NYE)
    scaling = jnp.take(element_coef, ordering).reshape(NXE, NYE)
    keep, weights = node_masks(jnp.arange(NXE), jnp.arange(NYE), NXE, NYE)

    def solve_mode(packed):
        fields, schur_mode, couple_mode, inner_mode = packed
        cycle_part = fields[:, :NB]
        inner_part = fields[:, NB:]
        condensed = cycle_part - jnp.einsum('mbi,mixy->mbxy', couple_mode, inner_part, precision=highest)
        residual = keep * assemble(condensed)

        def operator(search):
            return keep * assemble(scaling * jnp.einsum('mab,mbxy->maxy', schur_mode, search, precision=highest))

        def inner_sum(first, second):
            return lax.optimization_barrier(jnp.sum(weights * first * second, axis=(1, 2, 3)))[:, None, None, None]
        iterate = jnp.zeros_like(residual)
        search = residual
        norm_now = inner_sum(residual, residual)
        for sweep in range(ITERS):
            images = operator(search)
            step_size = norm_now / inner_sum(search, images)
            iterate = iterate + step_size * search
            residual = residual - step_size * images
            norm_next = inner_sum(residual, residual)
            search = residual + norm_next / norm_now * search
            norm_now = norm_next
        interior = jnp.einsum('mij,mjxy->mixy', inner_mode, inner_part, precision=highest) / scaling
        interior = interior - jnp.einsum('mbi,mbxy->mixy', couple_mode, iterate, precision=highest)
        return jnp.concatenate([iterate, interior], 1)
    modal = lax.map(solve_mode, (gridded[:, None], schur[:, None], couple[:, None], inner_inv[:, None]))
    modal = jnp.take(modal.reshape(NZ, NODES, ELEMENTS), location, axis=2)
    return jnp.einsum('jz,jne->zne', dft_table, modal, precision=highest)
```

```python
import functools
import math
import types

import jax
import jax.numpy as jnp
from jax import lax
from jax.experimental import pallas as pl
from jax.experimental.pallas import tpu as pltpu
from jax.sharding import PartitionSpec as P

P_SIZE = 8
ITERS = 3
ELX = 8
ELY = 16
NB = 4 * P_SIZE
NI = (P_SIZE - 1) ** 2
NODES = NB + NI
DEEP = 64
TALL = 56
LANES = 128
HIGHEST = lax.Precision.HIGHEST


def dft_values(row_index, plane_index, length):
    plane_pos = plane_index.astype(jnp.float32)
    waves = ((row_index + 1) // 2).astype(jnp.float32)
    angles = 2.0 * math.pi * waves * plane_pos / length
    factor = math.sqrt(2.0 / length)
    result = jnp.where(row_index % 2 == 1, factor * jnp.cos(angles), factor * jnp.sin(angles))
    result = jnp.where(row_index == 0, 1.0 / math.sqrt(length), result)
    return jnp.where(
        row_index == length - 1, jnp.cos(math.pi * plane_pos) / math.sqrt(length), result
    )


def stacked_table(values):
    high = lax.reduce_precision(values, 8, 7)
    low = values - high
    return jnp.concatenate([high, high, low], -1).astype(jnp.bfloat16)


def split(value):
    high = value.astype(jnp.bfloat16)
    return high, (value - high.astype(jnp.float32)).astype(jnp.bfloat16)


def dot(a, b):
    return jnp.dot(a, b, preferred_element_type=jnp.float32)


def product(a, b):
    (ah, al), (bh, bl) = split(a), split(b)
    rows = a.shape[0]
    both = dot(jnp.concatenate([ah, al], 0), bh)
    return both[:rows] + (both[rows:] + dot(ah, bl))


def pile(value):
    high, low = split(value)
    return jnp.concatenate([high, low, high], 0)


def aligned(start, size):
    return pl.ds(start if isinstance(start, int) else pl.multiple_of(start, size), size)


def loop(count, unroll, body):
    while count % unroll:
        unroll -= 1

    def step(outer, carry):
        for inner in range(unroll):
            body(outer * unroll + inner)
        return carry

    lax.fori_loop(0, count // unroll, step, 0)


class Plan:
    def __init__(self, sizes, modes, planes):
        self.groups, self.ex, self.ey = sizes
        self.modes, self.planes = modes, planes
        self.all_modes = self.groups * modes
        self.chunk = min(16, modes)
        self.chunks = modes // self.chunk
        self.fold = max(1, LANES // modes)
        self.couple_rows = NB // self.fold
        self.couple_ways = 2 if self.ey % 2 == 0 else 1
        step = 8 * self.couple_ways
        self.couple_part = -(-NI * self.couple_rows // step) * 8
        self.couple_all = max(DEEP * self.couple_rows, self.couple_part * self.couple_ways)
        self.inner_rows = -(-NI // self.fold)
        self.inner_ways = self.ey
        self.inner_part = -(-self.inner_rows * TALL // (8 * self.inner_ways)) * 8
        self.inner_all = self.inner_part * self.inner_ways
        self.peers = self.ex * self.ey - 1


def layout(p):
    f32 = lambda *dims: pltpu.VMEM(dims, jnp.float32)
    half = lambda *dims: pltpu.VMEM(dims, jnp.bfloat16)
    dma = lambda *dims: pltpu.SemaphoreType.DMA(dims)
    far, m, z = p.groups - 1, p.modes, p.planes
    field = f32(NB * m, LANES)
    rows = NB * p.chunk
    return dict(
        f=f32(NODES, z, LANES),
        fo=f32(far, NI, z, LANES),
        spec=f32((NB + DEEP) * p.all_modes, LANES),
        res=field,
        app=field,
        x=field,
        dir=field,
        along=field,
        cin=f32(NI, NB, m),
        sin=f32(NB, NB, m),
        iin=f32(NI, NI, m),
        cpack=f32(p.groups, p.couple_all, LANES),
        ipack=f32(p.groups, p.inner_all, LANES),
        cf=f32(p.all_modes * NB, LANES),
        ct=f32(p.all_modes * DEEP, LANES),
        invf=f32(p.all_modes * TALL, LANES),
        sch=f32(m * NB, LANES),
        cbuf=f32(rows, LANES),
        sbuf=f32(far, p.chunks, rows, LANES),
        rbuf=f32(far, p.chunks, rows, LANES),
        xe=f32(p.chunks, rows, LANES),
        xr=f32(far, p.chunks, rows, LANES),
        one=half(LANES, LANES),
        oneT=half(LANES, LANES),
        scale=f32(8, LANES),
        keep=f32(NB, LANES),
        weight=f32(NB, LANES),
        xs=f32(ITERS, 2, 2, m, LANES),
        xh=f32(ITERS, 2, 2, m, LANES),
        ys=f32(ITERS, 2, m, LANES),
        yh=f32(ITERS, 3, 2, m, LANES),
        ps=f32(ITERS, 1, 2 * m),
        pr=f32(ITERS, p.peers, 1, 2 * m),
        s_local=dma(5),
        s_halo=dma(2, ITERS, 8),
        s_sum=dma(2, ITERS, p.peers),
        s_cx=dma(2, far),
        s_cy=dma(2, far, max(1, p.couple_ways - 1)),
        s_ix=dma(2, far),
        s_iy=dma(2, far, max(1, p.inner_ways - 1)),
        s_f1=dma(2, far, p.chunks),
        s_f2=dma(2, far),
        s_b1=dma(2, far, p.chunks),
    )


def kernel(p, names, forcing, coef_ref, cell_ref, schur_in, couple_in, inner_in, fwd, back_own, back_far, out, *refs):
    s = types.SimpleNamespace(**dict(zip(names, refs)))
    m, z, gm, mc = p.modes, p.planes, p.all_modes, p.chunk
    cells = LANES
    sizes = {"fourier": p.groups, "ex": p.ex, "ey": p.ey}
    place = {axis: lax.axis_index(axis) for axis in sizes}
    lane = lax.broadcasted_iota(jnp.int32, (m, cells), 1)
    lane_row = lane // ELY
    lane_col = lane % ELY

    def shifted(axis, by):
        return lax.rem(place[axis] + (by % sizes[axis]), sizes[axis])

    def remote(source, target, sems, index, device):
        return pltpu.make_async_remote_copy(
            src_ref=source,
            dst_ref=target,
            send_sem=sems.at[(0,) + index],
            recv_sem=sems.at[(1,) + index],
            device_id=device,
            device_id_type=pl.DeviceIdType.MESH,
        )

    hops = range(1, p.groups)
    around = [(a, b) for a in range(p.ex) for b in range(p.ey) if a or b]

    loads = [
        pltpu.make_async_copy(couple_in, s.cin, s.s_local.at[0]),
        pltpu.make_async_copy(inner_in, s.iin, s.s_local.at[1]),
        pltpu.make_async_copy(
            forcing.at[pl.ds(NB, NI)], s.f.at[pl.ds(NB, NI)], s.s_local.at[2]
        ),
        pltpu.make_async_copy(forcing.at[pl.ds(0, NB)], s.f.at[pl.ds(0, NB)], s.s_local.at[3]),
        pltpu.make_async_copy(schur_in, s.sin, s.s_local.at[4]),
    ]
    for load in loads:
        load.start()

    s.xh[...] = jnp.zeros_like(s.xh)
    s.yh[...] = jnp.zeros_like(s.yh)

    barrier = pltpu.get_barrier_semaphore()
    for a, b in around:
        pl.semaphore_signal(
            barrier,
            inc=1,
            device_id={"ex": shifted("ex", a), "ey": shifted("ey", b)},
            device_id_type=pl.DeviceIdType.MESH,
        )
    for hop in hops:
        pl.semaphore_signal(
            barrier,
            inc=1,
            device_id={"fourier": shifted("fourier", hop)},
            device_id_type=pl.DeviceIdType.MESH,
        )

    def clear(ref, start, stop):
        if stop > start:
            ref[pl.ds(start, stop - start), :] = jnp.zeros((stop - start, LANES), jnp.float32)

    br = p.couple_rows
    own_rows = NI * br
    got_rows = p.couple_part * p.couple_ways
    clear(s.cpack.at[0], own_rows, p.couple_all)
    for g in hops:
        clear(s.cpack.at[g], got_rows, p.couple_all)
    loads[0].wait()
    for i in range(NI):
        s.cpack[0, i * br : (i + 1) * br, :] = jnp.concatenate(
            [s.cin[i, k * br : (k + 1) * br, :] for k in range(p.fold)], 1
        )
    pl.semaphore_wait(barrier, len(around) + p.groups - 1)

    def share_out(pack, part, ways, sem_x, sem_y):
        turn = lax.rem(place["ey"], ways)
        rows = aligned(turn * part, part) if part % 8 else pl.ds(pl.multiple_of(turn * part, 8), part)
        across = [
            remote(
                pack.at[0, rows], pack.at[g, rows], sem_x, (g - 1,),
                {"fourier": shifted("fourier", g)},
            )
            for g in hops
        ]
        beside = [
            remote(
                pack.at[g, rows], pack.at[g, rows], sem_y, (g - 1, k - 1),
                {"ey": place["ey"] - turn + lax.rem(turn + k, ways)},
            )
            for g in hops
            for k in range(1, ways)
        ]
        return across, beside

    couple_x, couple_y = share_out(s.cpack, p.couple_part, p.couple_ways, s.s_cx, s.s_cy)
    inner_x, inner_y = share_out(s.ipack, p.inner_part, p.inner_ways, s.s_ix, s.s_iy)
    for copy in couple_x:
        copy.start()

    loads[1].wait()
    ir = p.inner_rows
    clear(s.ipack.at[0], 0, p.inner_all)
    for i in range(ir):
        picks = [s.iin[min(k * ir + i, NI - 1), :, :] for k in range(p.fold)]
        s.ipack[0, i * TALL : i * TALL + NI, :] = jnp.concatenate(picks, 1)
    for copy in inner_x:
        copy.start()

    lines = lax.broadcasted_iota(jnp.int32, (LANES, LANES), 0)
    hot = jnp.where(lines == cell_ref[0:1, :], 1.0, 0.0).astype(jnp.float32)
    hot_t = jnp.transpose(hot)
    s.oneT[...] = hot.astype(jnp.bfloat16)
    s.one[...] = hot_t.astype(jnp.bfloat16)
    s.scale[...] = lax.dot_general(
        jnp.broadcast_to(coef_ref[0:1, :], (8, LANES)),
        hot_t,
        (((1,), (0,)), ((), ())),
        precision=HIGHEST,
        preferred_element_type=jnp.float32,
    )

    def flat(pack, g, start, count, stride, width):
        rows = pack[g, pl.ds(start, count, stride=stride) if stride > 1 else pl.ds(start, count), :]
        if count < LANES:
            rows = jnp.concatenate([rows, jnp.zeros((LANES - count, LANES), jnp.float32)], 0)
        return jnp.transpose(rows)

    def couple_matrices(g):
        for b in range(br):
            turned_rows = flat(s.cpack, g, b, DEEP, br, NI)
            for k in range(p.fold):
                s.cf[pl.ds(g * m * NB + k * br + b, m, stride=NB), :] = turned_rows[
                    k * m : (k + 1) * m
                ]

    def inner_matrices(g):
        for i in range(ir):
            turned_rows = flat(s.ipack, g, i * TALL, TALL, 1, NI)
            for k in range(p.fold):
                if k * ir + i < TALL:
                    s.invf[pl.ds(g * m * TALL + k * ir + i, m, stride=TALL), :] = turned_rows[
                        k * m : (k + 1) * m
                    ]

    def spectrum(n):
        s.spec[aligned(n * gm, gm), :] = dot(fwd[0], pile(s.f[n]))

    clear(s.spec, NODES * gm, (NB + DEEP) * gm)
    loads[2].wait()
    loop(NI, 7, lambda n: spectrum(NB + n))
    loads[3].wait()
    loop(NB, 8, spectrum)
    couple_matrices(0)

    def permuted(rows, hot_ref):
        high, low = split(rows)
        both = dot(jnp.concatenate([high, low], 0), hot_ref[...])
        return both[: rows.shape[0]] + both[rows.shape[0] :]

    def condense(g, c, store):
        def one_mode(k):
            j = g * m + c * mc + k
            inner = s.spec[pl.ds(NB * gm + j, DEEP, stride=gm), :]
            matrix = s.cf[aligned(j * NB, NB), :DEEP]
            s.cbuf[pl.ds(k, NB, stride=mc), :] = s.spec[
                pl.ds(j, NB, stride=gm), :
            ] - product(matrix, inner)

        loop(mc, 8, one_mode)
        for block in range(NB * mc // LANES):
            store(block, permuted(s.cbuf[block * LANES : (block + 1) * LANES, :], s.one))

    def keep_own(c):
        per = LANES // mc

        def store(block, rows):
            for k in range(per):
                n = block * per + k
                s.res[n * m + c * mc : n * m + (c + 1) * mc, :] = rows[k * mc : (k + 1) * mc]

        return store

    for copy in couple_x:
        copy.wait_recv()
    for copy in couple_y:
        copy.start()
    condense(0, 0, keep_own(0))
    for copy in couple_y:
        copy.wait_recv()

    first = []
    for g in hops:
        couple_matrices(g)
        for c in range(p.chunks):

            def store(block, rows, g=g, c=c):
                s.sbuf[g - 1, c, block * LANES : (block + 1) * LANES, :] = rows

            condense(g, c, store)
            copy = remote(
                s.sbuf.at[g - 1, c], s.rbuf.at[g - 1, c], s.s_f1, (g - 1, c),
                {"fourier": shifted("fourier", -g)},
            )
            copy.start()
            first.append((g, c, copy))

    second = []
    for g in hops:
        copy = remote(
            forcing.at[pl.ds(NB, NI)], s.fo.at[g - 1], s.s_f2, (g - 1,),
            {"fourier": shifted("fourier", g)},
        )
        copy.start()
        second.append(copy)
    for copy in inner_x:
        copy.wait_recv()
    for copy in inner_y:
        copy.start()

    for c in range(1, p.chunks):
        condense(0, c, keep_own(c))

    loads[4].wait()
    for a in range(NB):
        rows = s.sin[a]
        high = rows.astype(jnp.bfloat16).astype(jnp.float32)
        rows = jnp.concatenate([high, high, rows - high, jnp.zeros_like(rows)], 0)
        if m < LANES:
            rows = jnp.concatenate([rows, jnp.zeros((LANES, LANES - m), jnp.float32)], 1)
        s.sch[pl.ds(a, m, stride=NB), :] = jnp.transpose(rows)[:m]

    slots = lax.broadcasted_iota(jnp.int32, (NB, cells), 0)
    places = lax.broadcasted_iota(jnp.int32, (NB, cells), 1)
    row_ids = place["ex"] * ELX + places // ELY
    col_ids = place["ey"] * ELY + places % ELY
    dropped = (
        ((slots == 0) | (slots >= 3 * P_SIZE)) & (row_ids == 0)
        | (slots >= P_SIZE) & (slots <= 2 * P_SIZE) & (row_ids == ELX * p.ex - 1)
        | (slots <= P_SIZE) & (col_ids == 0)
        | (slots >= 2 * P_SIZE) & (slots <= 3 * P_SIZE) & (col_ids == ELY * p.ey - 1)
    )
    keep = jnp.where(dropped, 0.0, 1.0).astype(jnp.float32)
    s.keep[...] = keep
    s.weight[...] = keep * jnp.where(slots % P_SIZE == 0, 0.25, 0.5)
    for ref in (s.x, s.dir, s.along):
        ref[...] = jnp.zeros_like(ref)

    def couple_turned(q):
        square = jnp.transpose(s.cf[aligned(q * LANES, LANES), :])
        for k in range(LANES // NB):
            piece = square[:DEEP] if k == 0 else pltpu.roll(square[:DEEP], LANES - k * NB, 1)
            s.ct[aligned((q * (LANES // NB) + k) * DEEP, DEEP), :] = piece

    loop(gm * NB // LANES, 4, couple_turned)
    inner_matrices(0)
    for copy in inner_y:
        copy.wait_recv()
    for g in hops:
        inner_matrices(g)

    def node(n):
        return aligned(n * m, m)

    def turned(value, shift):
        shift = shift % cells
        return pltpu.roll(value, shift, 1) if shift else value

    def exists(axis, step):
        if step == 0:
            return None
        return place[axis] < sizes[axis] - 1 if step > 0 else place[axis] > 0

    def guarded(ex_step, ey_step, action):
        tests = [t for t in (exists("ex", ex_step), exists("ey", ey_step)) if t is not None]
        pl.when(functools.reduce(jnp.logical_and, tests))(action)

    def halo_copy(turn, number, source, target, ex_step, ey_step):
        copy = pltpu.make_async_remote_copy(
            src_ref=source,
            dst_ref=target,
            send_sem=s.s_halo.at[0, turn, number],
            recv_sem=s.s_halo.at[1, turn, number],
            device_id={"ex": shifted("ex", ex_step), "ey": shifted("ey", ey_step)},
            device_id_type=pl.DeviceIdType.MESH,
        )
        guarded(ex_step, ey_step, copy.start)
        return (
            lambda: guarded(-ex_step, -ey_step, copy.wait_recv),
            lambda: guarded(ex_step, ey_step, copy.wait_send),
        )

    def assemble(ref, turn):
        bottom = lambda k: k
        top = lambda k: 3 * P_SIZE - k
        left = lambda k: (NB - k) % NB
        right = lambda k: P_SIZE + k
        last = cells - ELY
        copies = []
        up = jnp.zeros((m, cells), jnp.float32)
        down = up
        for k in range(P_SIZE + 1):
            up = jnp.where(lane_col == k, turned(ref[node(top(k)), :], k - ELY + 1), up)
            down = jnp.where(lane_col == k, turned(ref[node(bottom(k)), :], k), down)
        s.ys[turn, 0] = up
        s.ys[turn, 1] = down
        for slot, ex_step in ((1, 1), (2, -1), (0, 0)):
            for way, ey_step in ((0, 1), (1, -1)):
                copies.append(
                    halo_copy(
                        turn, 2 * slot + way, s.ys.at[turn, way], s.yh.at[turn, slot, way],
                        ex_step, ey_step,
                    )
                )
        up = jnp.zeros((m, cells), jnp.float32)
        down = up
        for k in range(P_SIZE):
            up = jnp.where(lane_row == k, turned(ref[node(right(k)), :], ELY * k - last), up)
            down = jnp.where(lane_row == k, turned(ref[node(left(k)), :], ELY * k), down)
        s.xs[turn, 0, 0] = up
        s.xs[turn, 1, 0] = down
        s.xs[turn, 0, 1] = turned(ref[node(right(P_SIZE)), :], -last)
        s.xs[turn, 1, 1] = ref[node(left(P_SIZE)), :]
        for way, ex_step in ((0, 1), (1, -1)):
            copies.append(
                halo_copy(turn, 6 + way, s.xs.at[turn, way], s.xh.at[turn, way], ex_step, 0)
            )

        for k in range(P_SIZE + 1):
            here_left, here_right = ref[node(left(k)), :], ref[node(right(k)), :]
            ref[node(left(k)), :] = here_left + jnp.where(
                lane_row == 0, 0.0, turned(here_right, ELY)
            )
            ref[node(right(k)), :] = here_right + jnp.where(
                lane_row == ELX - 1, 0.0, turned(here_left, -ELY)
            )
        for arrive, _ in copies:
            arrive()

        for k in range(P_SIZE + 1):
            part, lanes = divmod(k, P_SIZE)
            low = turned(s.xh[turn, 0, part], -ELY * lanes)
            high = turned(s.xh[turn, 1, part], last - ELY * lanes)
            for n, halo, row in ((left(k), low, 0), (right(k), high, ELX - 1)):
                value = ref[node(n), :] + jnp.where(lane_row == row, halo, 0.0)
                if n % (2 * P_SIZE) > P_SIZE:
                    value = value * s.keep[n : n + 1, :]
                ref[node(n), :] = value

        lines = []
        for way in range(2):
            line = s.yh[turn, 0, way]
            before = jnp.where(
                lane == 0, turned(s.yh[turn, 1, way], P_SIZE), turned(line, P_SIZE)
            )
            after = jnp.where(
                lane == last + P_SIZE, turned(s.yh[turn, 2, way], -P_SIZE), turned(line, -P_SIZE)
            )
            lines.append(
                line
                + jnp.where(lane_col == 0, before, jnp.where(lane_col == P_SIZE, after, 0.0))
            )
        low_all, high_all = lines
        for k in range(P_SIZE + 1):
            b, t = bottom(k), top(k)
            here_bottom, here_top = ref[node(b), :], ref[node(t), :]
            ref[node(b), :] = s.keep[b : b + 1, :] * (
                here_bottom
                + jnp.where(lane_col == 0, turned(low_all, -k), turned(here_top, 1))
            )
            ref[node(t), :] = s.keep[t : t + 1, :] * (
                here_top
                + jnp.where(
                    lane_col == ELY - 1, turned(high_all, ELY - 1 - k), turned(here_bottom, -1)
                )
            )
        for _, leave in copies:
            leave()

    def operator():
        scale = s.scale[0:1, :]

        def one_mode(k):
            value = s.res[pl.ds(k, NB, stride=m), :]
            matrix = s.sch[aligned(k * NB, NB), : 3 * NB].astype(jnp.bfloat16)
            s.app[pl.ds(k, NB, stride=m), :] = dot(matrix, pile(value)) * scale

        loop(m, 8, one_mode)

    def sums_start(turn):
        def step(outer, sums):
            norm, curve = sums
            for inner in range(4):
                n = outer * 4 + inner
                mine = s.res[node(n), :]
                norm = norm + s.weight[pl.ds(n, 1), :] * mine * mine
                curve = curve + mine * s.app[node(n), :]
            return norm, curve

        zero = jnp.zeros((m, cells), jnp.float32)
        norm, curve = lax.fori_loop(0, NB // 4, step, (zero, zero))
        total = lax.dot_general(
            jnp.ones((8, cells), jnp.float32),
            jnp.concatenate([norm, curve], 0),
            (((1,), (1,)), ((), ())),
            precision=HIGHEST,
            preferred_element_type=jnp.float32,
        )
        s.ps[turn] = total[0:1, :]
        copies = [
            remote(
                s.ps.at[turn], s.pr.at[turn, k], s.s_sum, (turn, k),
                {"ex": shifted("ex", a), "ey": shifted("ey", b)},
            )
            for k, (a, b) in enumerate(around)
        ]
        for copy in copies:
            copy.start()
        return copies

    def sums_end(turn, copies):
        total = s.ps[turn]
        for k, copy in enumerate(copies):
            copy.wait_recv()
            total = total + s.pr[turn, k]
        for copy in copies:
            copy.wait_send()
        row = lax.broadcasted_iota(jnp.int32, (m, 2 * m), 0)
        column = lax.broadcasted_iota(jnp.int32, (m, 2 * m), 1)
        pick = lambda offset: jnp.sum(
            jnp.where(column == row + offset, total, 0.0), axis=1, keepdims=True
        )
        return pick(0), pick(m)

    for g, c, copy in first:
        copy.wait_recv()

        def add(n, g=g, c=c):
            rows = aligned(n * m + c * mc, mc)
            s.res[rows, :] = s.res[rows, :] + s.rbuf[g - 1, c, aligned(n * mc, mc), :]

        loop(NB, 8, add)
    assemble(s.res, 0)

    def scalars(turn, norm, curve, norm_before, step_before):
        ratio = jnp.where(turn == 0, 0.0, norm / norm_before)
        return ratio, norm / (curve - ratio * norm / step_before)

    def sweep(turn, carry):
        operator()
        copies = sums_start(turn)
        assemble(s.app, turn + 1)
        norm, curve = sums_end(turn, copies)
        ratio, step_size = scalars(turn, norm, curve, *carry)

        def update(n):
            rows = node(n)
            search = s.res[rows, :] + ratio * s.dir[rows, :]
            along = s.app[rows, :] + ratio * s.along[rows, :]
            s.x[rows, :] = s.x[rows, :] + step_size * search
            s.dir[rows, :] = search
            s.along[rows, :] = along
            s.res[rows, :] = s.res[rows, :] - step_size * along

        loop(NB, 4, update)
        return norm, step_size

    one = jnp.ones((m, 1), jnp.float32)
    carry = lax.fori_loop(0, ITERS - 1, sweep, (one, one))
    operator()
    norm, curve = sums_end(ITERS - 1, sums_start(ITERS - 1))
    ratio, step_size = scalars(ITERS - 1, norm, curve, *carry)

    def finish(n):
        rows = node(n)
        s.x[rows, :] = s.x[rows, :] + step_size * (s.res[rows, :] + ratio * s.dir[rows, :])

    loop(NB, 4, finish)

    per = LANES // mc
    third = []
    for c in range(p.chunks):
        for block in range(NB // per):
            rows = jnp.concatenate(
                [
                    s.x[n * m + c * mc : n * m + (c + 1) * mc, :]
                    for n in range(block * per, (block + 1) * per)
                ],
                0,
            )
            s.xe[c, block * LANES : (block + 1) * LANES, :] = permuted(rows, s.oneT)
        for g in hops:
            copy = remote(
                s.xe.at[c], s.xr.at[g - 1, c], s.s_b1, (g - 1, c),
                {"fourier": shifted("fourier", g)},
            )
            copy.start()
            third.append((g, c, copy))

    for copy in second:
        copy.wait_recv()

    def add_far(n):
        rows = aligned((NB + n) * gm, gm)
        total = s.spec[rows, :]
        for g in hops:
            total = total + dot(fwd[g], pile(s.fo[g - 1, n]))
        s.spec[rows, :] = total

    loop(NI, 7, add_far)
    inverse_coef = 1.0 / coef_ref[0:1, :]

    def base(j):
        inner = s.spec[pl.ds(NB * gm + j, DEEP, stride=gm), :]
        matrix = s.invf[pl.ds(pl.multiple_of(j * TALL, 8), TALL), :DEEP]
        value = product(matrix, inner) * inverse_coef
        s.spec[pl.ds(NB * gm + j, NI, stride=gm), :] = value[:NI]

    loop(gm, 4, base)

    def place_cycle(g, c, source):
        def interior(k):
            j = g * m + c * mc + k
            matrix = s.ct[aligned(j * DEEP, DEEP), :NB]
            value = product(matrix, source[pl.ds(k, NB, stride=mc), :])
            rows = pl.ds(NB * gm + j, NI, stride=gm)
            s.spec[rows, :] = s.spec[rows, :] - value[:NI]

        loop(mc, 4, interior)

        def cycle(n):
            s.spec[aligned(n * gm + g * m + c * mc, mc), :] = source[aligned(n * mc, mc), :]

        loop(NB, 8, cycle)

    for c in range(p.chunks):
        place_cycle(0, c, s.xe.at[c])

    def own_velocity(n):
        out[n] = dot(back_own[...], pile(s.spec[aligned(n * gm, m), :]))

    loop(NODES, 9, own_velocity)

    for g, c, copy in third:
        copy.wait_recv()
        place_cycle(g, c, s.xr.at[g - 1, c])

        def far_velocity(n, g=g, c=c):
            rows = s.spec[aligned(n * gm + g * m + c * mc, mc), :]
            out[n] = out[n] + dot(back_far[(g - 1) * p.chunks + c], pile(rows))

        loop(NODES, 9, far_velocity)

    for copy in couple_x + couple_y + inner_x + inner_y + second:
        copy.wait_send()
    for _, _, copy in first + third:
        copy.wait_send()


def on_device(forcing, element_coef, schur, couple, inner_inv, element_cell):
    planes, _, elements = forcing.shape
    modes = schur.shape[0]
    sizes = tuple(lax.axis_size(axis) for axis in ("fourier", "ex", "ey"))
    p = Plan(sizes, modes, planes)
    me = lax.axis_index("fourier")
    length = planes * p.groups

    def group_of(hop):
        return lax.rem(me + p.groups - hop, p.groups)

    def iota(shape, dim):
        return lax.broadcasted_iota(jnp.int32, shape, dim)

    dims = (p.groups, p.all_modes, planes)
    mode = group_of(iota(dims, 1) // modes) * modes + iota(dims, 1) % modes
    plane = group_of(iota(dims, 0)) * planes + iota(dims, 2)
    fwd = stacked_table(dft_values(mode, plane, length))
    dims = (planes, modes)
    back_own = stacked_table(
        dft_values(me * modes + iota(dims, 1), me * planes + iota(dims, 0), length)
    )
    dims = ((p.groups - 1) * p.chunks, planes, p.chunk)
    hop = 1 + iota(dims, 0) // p.chunks
    mode = group_of(hop) * modes + iota(dims, 0) % p.chunks * p.chunk + iota(dims, 2)
    back_far = stacked_table(dft_values(mode, me * planes + iota(dims, 1), length))

    scratch = layout(p)
    whole = pl.BlockSpec(memory_space=pltpu.VMEM)
    stay = pl.BlockSpec(memory_space=pl.ANY)
    velocity = pl.pallas_call(
        functools.partial(kernel, p, tuple(scratch)),
        out_shape=jax.ShapeDtypeStruct((NODES, planes, elements), jnp.float32),
        in_specs=[stay, whole, whole, stay, stay, stay, whole, whole, whole],
        out_specs=whole,
        scratch_shapes=list(scratch.values()),
        compiler_params=pltpu.CompilerParams(
            collective_id=0, has_side_effects=True, vmem_limit_bytes=60 << 20
        ),
        cost_estimate=pl.CostEstimate(flops=10**9, bytes_accessed=2 * 10**8, transcendentals=0),
    )(
        jnp.transpose(forcing, (1, 0, 2)),
        element_coef[None],
        element_cell[None],
        jnp.transpose(schur, (1, 2, 0)),
        jnp.transpose(couple, (2, 1, 0)),
        jnp.transpose(inner_inv, (1, 2, 0)),
        fwd,
        back_own,
        back_far,
    )
    return jnp.transpose(velocity, (1, 0, 2))


def solution(mesh):
    placed = (
        P("fourier", None, ("ex", "ey")),
        P(("ex", "ey")),
        P("fourier", None, None),
        P("fourier", None, None),
        P("fourier", None, None),
        P(("ex", "ey")),
    )
    return jax.shard_map(
        on_device,
        mesh=mesh,
        in_specs=placed,
        out_specs=P("fourier", None, ("ex", "ey")),
        check_vma=False,
    )
```

```python
import functools
import math
import types

import jax
import jax.numpy as jnp
from jax import lax
from jax.experimental import pallas as pl
from jax.experimental.pallas import tpu as pltpu
from jax.sharding import PartitionSpec as P

P_SIZE = 8
ITERS = 3
ELX = 8
ELY = 16
NB = 4 * P_SIZE
NI = (P_SIZE - 1) ** 2
NODES = NB + NI
DEEP = 64
TALL = 56
LANES = 128
PLANES = 2 * P_SIZE + 1
HIGHEST = lax.Precision.HIGHEST


def dft_values(row_index, plane_index, length):
    plane_pos = plane_index.astype(jnp.float32)
    waves = ((row_index + 1) // 2).astype(jnp.float32)
    angles = 2.0 * math.pi * waves * plane_pos / length
    factor = math.sqrt(2.0 / length)
    result = jnp.where(row_index % 2 == 1, factor * jnp.cos(angles), factor * jnp.sin(angles))
    result = jnp.where(row_index == 0, 1.0 / math.sqrt(length), result)
    return jnp.where(
        row_index == length - 1, jnp.cos(math.pi * plane_pos) / math.sqrt(length), result
    )


def stacked(values):
    high = values.astype(jnp.bfloat16).astype(jnp.float32)
    return jnp.concatenate([high, high, values - high], 1).astype(jnp.bfloat16)


def split(value):
    high = value.astype(jnp.bfloat16)
    return high, (value - high.astype(jnp.float32)).astype(jnp.bfloat16)


def dot(a, b):
    return jnp.dot(a, b, preferred_element_type=jnp.float32)


def product(a, b):
    (ah, al), (bh, bl) = split(a), split(b)
    rows = a.shape[0]
    both = dot(jnp.concatenate([ah, al], 0), bh)
    return both[:rows] + (both[rows:] + dot(ah, bl))


def pile(value):
    high, low = split(value)
    return jnp.concatenate([high, low, high], 0)


def aligned(start, size):
    return pl.ds(start if isinstance(start, int) else pl.multiple_of(start, size), size)


def tile(start, size):
    return pl.ds(start if isinstance(start, int) else pl.multiple_of(start, 8), size)


def loop(count, unroll, body):
    while count % unroll:
        unroll -= 1

    def step(outer, carry):
        for inner in range(unroll):
            body(outer * unroll + inner)
        return carry

    lax.fori_loop(0, count // unroll, step, 0)


class Plan:
    def __init__(self, sizes, modes, planes):
        self.groups, self.ex, self.ey = sizes
        self.modes, self.planes = modes, planes
        self.all_modes = self.groups * modes
        self.chunk = min(16, modes)
        self.chunks = modes // self.chunk
        self.part = min(32, modes)
        self.parts = modes // self.part
        self.part_pitch = self.part + 8
        self.fold = max(1, LANES // modes)
        self.couple_rows = NB // self.fold
        self.couple_ways = self.ey
        step = 8 * self.couple_ways
        self.couple_part = -(-NI * self.couple_rows // step) * 8
        self.couple_all = max(DEEP * self.couple_rows, self.couple_part * self.couple_ways)
        self.inner_rows = -(-NI // self.fold)
        self.inner_ways = self.ex * self.ey
        self.inner_part = -(-self.inner_rows * TALL // (8 * self.inner_ways)) * 8
        self.inner_all = self.inner_part * self.inner_ways
        self.peers = self.ex * self.ey - 1
        self.pitch = modes + 8
        self.all_pitch = self.all_modes + 8
        self.chunk_pitch = self.chunk + 8
        self.matrix = NB + 8


def layout(p):
    f32 = lambda *dims: pltpu.VMEM(dims, jnp.float32)
    half = lambda *dims: pltpu.VMEM(dims, jnp.bfloat16)
    dma = lambda *dims: pltpu.SemaphoreType.DMA(dims)
    far, m, z = p.groups - 1, p.modes, p.planes
    field = f32(NB * p.pitch, LANES)
    return dict(
        f=f32(NODES, z, LANES),
        fo=f32(far, NI, z, LANES),
        spec=f32((NB + DEEP) * p.all_pitch, LANES),
        res=field,
        app=field,
        x=field,
        dir=field,
        along=field,
        cin=f32(NI, NB, m),
        sin=f32(NB, NB, m),
        iin=f32(NI, NI, m),
        cpack=f32(p.groups, p.couple_all, LANES),
        ipack=f32(p.groups, p.inner_all, LANES),
        cf=f32(p.all_modes * p.matrix, LANES),
        ct=f32(p.all_modes * DEEP, LANES),
        invf=f32(p.all_modes * TALL, LANES),
        sch=f32(m * p.matrix, LANES),
        cbuf=f32(NB * p.chunk_pitch, LANES),
        cgrid=f32(NB * p.chunk, LANES),
        sbuf=f32(far, p.chunks, PLANES * p.chunk, LANES),
        rbuf=f32(far, p.chunks, PLANES * p.chunk, LANES),
        xe=f32(NB * p.part_pitch, LANES),
        xsend=f32(p.parts, PLANES * p.part, LANES),
        xr=f32(far, p.parts, PLANES * p.part, LANES),
        fwd=half(p.groups, p.all_modes, 3 * z),
        back=half(z, 3 * m),
        far=half(far * p.parts, z, 3 * p.part),
        one=half(LANES, LANES),
        oneT=half(LANES, LANES),
        scale=f32(8, LANES),
        coef=f32(1, LANES),
        cell=pltpu.VMEM((1, LANES), jnp.int32),
        keep=f32(NB, LANES),
        weight=f32(NB, LANES),
        xs=f32(ITERS, 2, 2, m, LANES),
        xh=f32(ITERS, 2, 2, m, LANES),
        ys=f32(ITERS, 2, m, LANES),
        yh=f32(ITERS, 3, 2, m, LANES),
        ps=f32(ITERS, 1, 2 * m),
        pr=f32(ITERS, p.peers, 1, 2 * m),
        s_local=dma(7),
        s_halo=dma(2, ITERS, 8),
        s_sum=dma(2, ITERS, p.peers),
        s_couple=dma(2, 2, far, max(1, p.ey - 1)),
        s_inner=dma(2, 3, far, max(1, p.ex - 1, p.ey - 1)),
        s_f1=dma(2, far, p.chunks),
        s_f2=dma(2, far, 4),
        s_b1=dma(2, far, p.parts),
    )


def kernel(p, names, forcing, coef_in, cell_in, schur_in, couple_in, inner_in, table, out, *refs):
    s = types.SimpleNamespace(**dict(zip(names, refs)))
    m, z, gm, mc = p.modes, p.planes, p.all_modes, p.chunk
    mp, gp, cp, nb = p.pitch, p.all_pitch, p.chunk_pitch, p.matrix
    mo, op = p.part, p.part_pitch
    cells = LANES
    sizes = {"fourier": p.groups, "ex": p.ex, "ey": p.ey}
    place = {axis: lax.axis_index(axis) for axis in sizes}
    lane = lax.broadcasted_iota(jnp.int32, (m, cells), 1)
    lane_row = lane // ELY
    lane_col = lane % ELY

    def shifted(axis, by):
        return lax.rem(place[axis] + (by % sizes[axis]), sizes[axis])

    def remote(source, target, sems, index, device):
        return pltpu.make_async_remote_copy(
            src_ref=source,
            dst_ref=target,
            send_sem=sems.at[(0,) + index],
            recv_sem=sems.at[(1,) + index],
            device_id=device,
            device_id_type=pl.DeviceIdType.MESH,
        )

    hops = range(1, p.groups)
    around = [(a, b) for a in range(p.ex) for b in range(p.ey) if a or b]

    bottom = lambda k: k
    top = lambda k: 3 * P_SIZE - k
    left = lambda k: (NB - k) % NB
    right = lambda k: P_SIZE + k
    last = cells - ELY

    def turned(value, shift):
        shift = shift % cells
        return pltpu.roll(value, shift, 1) if shift else value

    def grid(rows):
        where = lax.broadcasted_iota(jnp.int32, (rows, cells), 1)
        return where // ELY, where % ELY

    def compress(load, store, rows):
        row, col = grid(rows)

        def sideways(k):
            return load(left(k)) + jnp.where(row == 0, 0.0, turned(load(right(k)), ELY))

        corner = sideways(P_SIZE)
        store(0, sideways(0) + jnp.where(col == 0, 0.0, turned(corner, 1)))
        for k in range(1, P_SIZE):
            store(k, load(k) + jnp.where(col == 0, 0.0, turned(load(top(k)), 1)))
            store(P_SIZE - 1 + k, sideways(k))
        edge = load(right(0)) + jnp.where(col == 0, 0.0, turned(load(right(P_SIZE)), 1))
        far_row = turned(edge, -last)
        far_col = turned(corner, 1 - ELY)
        for k in range(1, P_SIZE):
            far_row = jnp.where(row == k, turned(load(right(k)), ELY * k - last), far_row)
            far_col = jnp.where(col == k, turned(load(top(k)), k - ELY + 1), far_col)
        tip = turned(load(top(P_SIZE)), P_SIZE - ELY + 1)
        store(2 * P_SIZE - 1, far_row)
        store(
            2 * P_SIZE,
            jnp.where(
                col < P_SIZE,
                far_col,
                jnp.where((col == P_SIZE) & (row == ELX - 1), tip, 0.0),
            ),
        )

    def pick_planes(load, store, rows):
        row, col = grid(rows)
        far_row = turned(load(right(0)), -last)
        far_col = turned(load(top(0)), 1 - ELY)
        for k in range(P_SIZE):
            store(k, load(k))
        for k in range(1, P_SIZE):
            store(P_SIZE - 1 + k, load(left(k)))
            far_row = jnp.where(row == k, turned(load(right(k)), ELY * k - last), far_row)
        for k in range(1, P_SIZE + 1):
            far_col = jnp.where(col == k, turned(load(top(k)), k - ELY + 1), far_col)
        store(2 * P_SIZE - 1, far_row)
        store(2 * P_SIZE, far_col)

    def spread(load, n, rows, inside):
        row, col = grid(rows)
        if n < P_SIZE:
            return load(n)
        if n > 3 * P_SIZE:
            return load(P_SIZE - 1 + NB - n)
        if n < 2 * P_SIZE:
            k = n - P_SIZE
            beside = turned(load(k and P_SIZE - 1 + k), -ELY) if inside else 0.0
            return jnp.where(
                row == ELX - 1, turned(load(2 * P_SIZE - 1), last - ELY * k), beside
            )
        k = 3 * P_SIZE - n
        if inside:
            above = turned(load(k) if k < P_SIZE else spread(load, P_SIZE, rows, True), -1)
        else:
            above = 0.0
        return jnp.where(col == ELY - 1, turned(load(2 * P_SIZE), ELY - 1 - k), above)

    def planes_of(ref, rows):
        return lambda k: ref[k * rows : (k + 1) * rows, :]

    loads = [
        pltpu.make_async_copy(couple_in, s.cin, s.s_local.at[0]),
        pltpu.make_async_copy(inner_in, s.iin, s.s_local.at[1]),
        pltpu.make_async_copy(
            forcing.at[pl.ds(NB, NI)], s.f.at[pl.ds(NB, NI)], s.s_local.at[2]
        ),
        pltpu.make_async_copy(forcing.at[pl.ds(0, NB)], s.f.at[pl.ds(0, NB)], s.s_local.at[3]),
        pltpu.make_async_copy(schur_in, s.sin, s.s_local.at[4]),
        pltpu.make_async_copy(coef_in, s.coef, s.s_local.at[5]),
        pltpu.make_async_copy(cell_in, s.cell, s.s_local.at[6]),
    ]
    for load in loads:
        load.start()

    s.xh[...] = jnp.zeros_like(s.xh)
    s.yh[...] = jnp.zeros_like(s.yh)

    barrier = pltpu.get_barrier_semaphore()
    for a, b in around:
        pl.semaphore_signal(
            barrier,
            inc=1,
            device_id={"ex": shifted("ex", a), "ey": shifted("ey", b)},
            device_id_type=pl.DeviceIdType.MESH,
        )
    for hop in hops:
        pl.semaphore_signal(
            barrier,
            inc=1,
            device_id={"fourier": shifted("fourier", hop)},
            device_id_type=pl.DeviceIdType.MESH,
        )

    def clear(ref, start, stop):
        if stop > start:
            ref[pl.ds(start, stop - start), :] = jnp.zeros((stop - start, LANES), jnp.float32)

    br = p.couple_rows
    own_rows = NI * br
    got_rows = p.couple_part * p.couple_ways
    clear(s.cpack.at[0], own_rows, p.couple_all)
    for g in hops:
        clear(s.cpack.at[g], got_rows, p.couple_all)
    loads[0].wait()
    for i in range(NI):
        s.cpack[0, i * br : (i + 1) * br, :] = jnp.concatenate(
            [s.cin[i, k * br : (k + 1) * br, :] for k in range(p.fold)], 1
        )
    pl.semaphore_wait(barrier, len(around) + p.groups - 1)

    def share_out(pack, part, over_ex, sems):
        turn = place["ey"] * p.ex + place["ex"] if over_ex else place["ey"]
        rows = tile(turn * part, part)
        stages = [
            [
                remote(
                    pack.at[0, rows], pack.at[g, rows], sems, (0, g - 1, 0),
                    {"fourier": shifted("fourier", g)},
                )
                for g in hops
            ]
        ]
        for axis in ("ex", "ey") if over_ex else ("ey",):
            if over_ex and axis == "ey":
                rows = tile(place["ey"] * p.ex * part, p.ex * part)
            stages.append(
                [
                    remote(
                        pack.at[g, rows], pack.at[g, rows], sems, (len(stages), g - 1, k - 1),
                        {axis: shifted(axis, k)},
                    )
                    for g in hops
                    for k in range(1, sizes[axis])
                ]
            )
        return stages

    def start(stage):
        for copy in stage:
            copy.start()

    def arrive(stage):
        for copy in stage:
            copy.wait_recv()

    couple = share_out(s.cpack, p.couple_part, False, s.s_couple)
    inner_parts = share_out(s.ipack, p.inner_part, True, s.s_inner)
    start(couple[0])

    loads[1].wait()
    ir = p.inner_rows
    clear(s.ipack.at[0], 0, p.inner_all)
    for i in range(ir):
        picks = [s.iin[min(k * ir + i, NI - 1), :, :] for k in range(p.fold)]
        s.ipack[0, i * TALL : i * TALL + NI, :] = jnp.concatenate(picks, 1)
    start(inner_parts[0])

    bounds = [0, NI // 7, NI * 3 // 7, NI * 5 // 7, NI]
    second = [
        [
            remote(
                forcing.at[pl.ds(NB + a, b - a)], s.fo.at[g - 1, pl.ds(a, b - a)], s.s_f2,
                (g - 1, k), {"fourier": shifted("fourier", g)},
            )
            for g in hops
        ]
        for k, (a, b) in enumerate(zip(bounds, bounds[1:]))
    ]
    start(second[0])

    for g in range(p.groups):
        s.fwd[g] = stacked(table[:, g * z : (g + 1) * z])
    flipped = jnp.transpose(table[...])[:z]
    s.back[...] = stacked(flipped[:, :m])
    for k in range((p.groups - 1) * p.parts):
        s.far[k] = stacked(flipped[:, m + k * mo : m + (k + 1) * mo])

    loads[5].wait()
    loads[6].wait()
    lines = lax.broadcasted_iota(jnp.int32, (LANES, LANES), 0)
    hot = jnp.where(lines == s.cell[...], 1.0, 0.0).astype(jnp.float32)
    hot_t = jnp.transpose(hot)
    s.oneT[...] = hot.astype(jnp.bfloat16)
    s.one[...] = hot_t.astype(jnp.bfloat16)
    s.scale[...] = lax.dot_general(
        jnp.broadcast_to(s.coef[...], (8, LANES)),
        hot_t,
        (((1,), (0,)), ((), ())),
        precision=HIGHEST,
        preferred_element_type=jnp.float32,
    )

    def flat(pack, g, start, count, stride, width):
        rows = pack[g, pl.ds(start, count, stride=stride) if stride > 1 else pl.ds(start, count), :]
        if count < LANES:
            rows = jnp.concatenate([rows, jnp.zeros((LANES - count, LANES), jnp.float32)], 0)
        return jnp.transpose(rows)

    def couple_matrices(g):
        for b in range(br):
            turned_rows = flat(s.cpack, g, b, DEEP, br, NI)
            for k in range(p.fold):
                s.cf[pl.ds(g * m * nb + k * br + b, m, stride=nb), :] = turned_rows[
                    k * m : (k + 1) * m
                ]

    def inner_matrices(g):
        for i in range(ir):
            turned_rows = flat(s.ipack, g, i * TALL, TALL, 1, NI)
            for k in range(p.fold):
                if k * ir + i < TALL:
                    s.invf[pl.ds(g * m * TALL + k * ir + i, m, stride=TALL), :] = turned_rows[
                        k * m : (k + 1) * m
                    ]

    def spectrum(n):
        s.spec[tile(n * gp, gm), :] = dot(s.fwd[0], pile(s.f[n]))

    clear(s.spec, NODES * gp, (NB + DEEP) * gp)
    loads[2].wait()
    loop(NI, 7, lambda n: spectrum(NB + n))
    loads[3].wait()
    loop(NB, 8, spectrum)
    couple_matrices(0)

    def permuted(rows, hot_ref):
        high, low = split(rows)
        both = dot(jnp.concatenate([high, low], 0), hot_ref[...])
        return both[: rows.shape[0]] + both[rows.shape[0] :]

    def condense(g, c, store):
        def one_mode(k):
            j = g * m + c * mc + k
            inner = s.spec[pl.ds(NB * gp + j, DEEP, stride=gp), :]
            matrix = s.cf[tile(j * nb, NB), :DEEP]
            s.cbuf[pl.ds(k, NB, stride=cp), :] = s.spec[
                pl.ds(j, NB, stride=gp), :
            ] - product(matrix, inner)

        loop(mc, 8, one_mode)
        for block in range(NB * mc // LANES):
            rows = [
                s.cbuf[n * cp : n * cp + mc, :]
                for n in range(block * (LANES // mc), (block + 1) * (LANES // mc))
            ]
            store(block, permuted(jnp.concatenate(rows, 0), s.one))

    def keep_own(c):
        per = LANES // mc

        def store(block, rows):
            for k in range(per):
                n = block * per + k
                s.res[n * mp + c * mc : n * mp + (c + 1) * mc, :] = rows[k * mc : (k + 1) * mc]

        return store

    arrive(couple[0])
    start(couple[1])
    arrive(inner_parts[0])
    start(inner_parts[1])
    early = p.chunks // 2
    for c in range(early):
        condense(0, c, keep_own(c))
    arrive(couple[1])

    first = []
    for g in hops:
        couple_matrices(g)
        for c in range(p.chunks):

            def store(block, rows):
                s.cgrid[block * LANES : (block + 1) * LANES, :] = rows

            condense(g, c, store)

            def put(k, value, g=g, c=c):
                s.sbuf[g - 1, c, k * mc : (k + 1) * mc, :] = value

            compress(planes_of(s.cgrid, mc), put, mc)
            copy = remote(
                s.sbuf.at[g - 1, c], s.rbuf.at[g - 1, c], s.s_f1, (g - 1, c),
                {"fourier": shifted("fourier", -g)},
            )
            copy.start()
            first.append((g, c, copy))

    for stage in second[1:]:
        start(stage)
    arrive(inner_parts[1])
    start(inner_parts[2])

    for c in range(early, p.chunks):
        condense(0, c, keep_own(c))

    loads[4].wait()
    for a in range(NB):
        rows = s.sin[a]
        high = rows.astype(jnp.bfloat16).astype(jnp.float32)
        rows = jnp.concatenate([high, high, rows - high, jnp.zeros_like(rows)], 0)
        if m < LANES:
            rows = jnp.concatenate([rows, jnp.zeros((LANES, LANES - m), jnp.float32)], 1)
        s.sch[pl.ds(a, m, stride=nb), :] = jnp.transpose(rows)[:m]

    slots = lax.broadcasted_iota(jnp.int32, (NB, cells), 0)
    places = lax.broadcasted_iota(jnp.int32, (NB, cells), 1)
    row_ids = place["ex"] * ELX + places // ELY
    col_ids = place["ey"] * ELY + places % ELY
    dropped = (
        ((slots == 0) | (slots >= 3 * P_SIZE)) & (row_ids == 0)
        | (slots >= P_SIZE) & (slots <= 2 * P_SIZE) & (row_ids == ELX * p.ex - 1)
        | (slots <= P_SIZE) & (col_ids == 0)
        | (slots >= 2 * P_SIZE) & (slots <= 3 * P_SIZE) & (col_ids == ELY * p.ey - 1)
    )
    keep = jnp.where(dropped, 0.0, 1.0).astype(jnp.float32)
    s.keep[...] = keep
    s.weight[...] = keep * jnp.where(slots % P_SIZE == 0, 0.25, 0.5)

    def couple_turned(q):
        rows = [s.cf[tile((q * (LANES // NB) + k) * nb, NB), :] for k in range(LANES // NB)]
        square = jnp.transpose(jnp.concatenate(rows, 0))
        for k in range(LANES // NB):
            piece = square[:DEEP] if k == 0 else pltpu.roll(square[:DEEP], LANES - k * NB, 1)
            s.ct[aligned((q * (LANES // NB) + k) * DEEP, DEEP), :] = piece

    loop(gm * NB // LANES, 4, couple_turned)
    inner_matrices(0)
    arrive(inner_parts[2])
    for g in hops:
        inner_matrices(g)

    def node(n):
        return tile(n * mp, m)

    def exists(axis, step):
        if step == 0:
            return None
        return place[axis] < sizes[axis] - 1 if step > 0 else place[axis] > 0

    def guarded(ex_step, ey_step, action):
        tests = [t for t in (exists("ex", ex_step), exists("ey", ey_step)) if t is not None]
        pl.when(functools.reduce(jnp.logical_and, tests))(action)

    def halo_copy(turn, number, source, target, ex_step, ey_step):
        copy = pltpu.make_async_remote_copy(
            src_ref=source,
            dst_ref=target,
            send_sem=s.s_halo.at[0, turn, number],
            recv_sem=s.s_halo.at[1, turn, number],
            device_id={"ex": shifted("ex", ex_step), "ey": shifted("ey", ey_step)},
            device_id_type=pl.DeviceIdType.MESH,
        )
        guarded(ex_step, ey_step, copy.start)
        return (
            lambda: guarded(-ex_step, -ey_step, copy.wait_recv),
            lambda: guarded(ex_step, ey_step, copy.wait_send),
        )

    def assemble(ref, turn, meanwhile):
        copies = []
        up = jnp.zeros((m, cells), jnp.float32)
        down = up
        for k in range(P_SIZE + 1):
            up = jnp.where(lane_col == k, turned(ref[node(top(k)), :], k - ELY + 1), up)
            down = jnp.where(lane_col == k, turned(ref[node(bottom(k)), :], k), down)
        s.ys[turn, 0] = up
        s.ys[turn, 1] = down
        for slot, ex_step in ((1, 1), (2, -1), (0, 0)):
            for way, ey_step in ((0, 1), (1, -1)):
                copies.append(
                    halo_copy(
                        turn, 2 * slot + way, s.ys.at[turn, way], s.yh.at[turn, slot, way],
                        ex_step, ey_step,
                    )
                )
        up = jnp.zeros((m, cells), jnp.float32)
        down = up
        for k in range(P_SIZE):
            up = jnp.where(lane_row == k, turned(ref[node(right(k)), :], ELY * k - last), up)
            down = jnp.where(lane_row == k, turned(ref[node(left(k)), :], ELY * k), down)
        s.xs[turn, 0, 0] = up
        s.xs[turn, 1, 0] = down
        s.xs[turn, 0, 1] = turned(ref[node(right(P_SIZE)), :], -last)
        s.xs[turn, 1, 1] = ref[node(left(P_SIZE)), :]
        for way, ex_step in ((0, 1), (1, -1)):
            copies.append(
                halo_copy(turn, 6 + way, s.xs.at[turn, way], s.xh.at[turn, way], ex_step, 0)
            )

        for k in range(P_SIZE + 1):
            here_left, here_right = ref[node(left(k)), :], ref[node(right(k)), :]
            ref[node(left(k)), :] = here_left + jnp.where(
                lane_row == 0, 0.0, turned(here_right, ELY)
            )
            ref[node(right(k)), :] = here_right + jnp.where(
                lane_row == ELX - 1, 0.0, turned(here_left, -ELY)
            )
        meanwhile()
        for wait, _ in copies:
            wait()

        for k in range(P_SIZE + 1):
            part, lanes = divmod(k, P_SIZE)
            low = turned(s.xh[turn, 0, part], -ELY * lanes)
            high = turned(s.xh[turn, 1, part], last - ELY * lanes)
            for n, halo, row in ((left(k), low, 0), (right(k), high, ELX - 1)):
                value = ref[node(n), :] + jnp.where(lane_row == row, halo, 0.0)
                if n % (2 * P_SIZE) > P_SIZE:
                    value = value * s.keep[n : n + 1, :]
                ref[node(n), :] = value

        lines = []
        for way in range(2):
            line = s.yh[turn, 0, way]
            before = jnp.where(
                lane == 0, turned(s.yh[turn, 1, way], P_SIZE), turned(line, P_SIZE)
            )
            after = jnp.where(
                lane == last + P_SIZE, turned(s.yh[turn, 2, way], -P_SIZE), turned(line, -P_SIZE)
            )
            lines.append(
                line
                + jnp.where(lane_col == 0, before, jnp.where(lane_col == P_SIZE, after, 0.0))
            )
        low_all, high_all = lines
        for k in range(P_SIZE + 1):
            b, t = bottom(k), top(k)
            here_bottom, here_top = ref[node(b), :], ref[node(t), :]
            ref[node(b), :] = s.keep[b : b + 1, :] * (
                here_bottom
                + jnp.where(lane_col == 0, turned(low_all, -k), turned(here_top, 1))
            )
            ref[node(t), :] = s.keep[t : t + 1, :] * (
                here_top
                + jnp.where(
                    lane_col == ELY - 1, turned(high_all, ELY - 1 - k), turned(here_bottom, -1)
                )
            )
        for _, leave in copies:
            leave()

    def operator():
        scale = s.scale[0:1, :]

        def one_mode(k):
            value = s.res[pl.ds(k, NB, stride=mp), :]
            matrix = s.sch[tile(k * nb, NB), : 3 * NB].astype(jnp.bfloat16)
            s.app[pl.ds(k, NB, stride=mp), :] = dot(matrix, pile(value)) * scale

        loop(m, 8, one_mode)

    def sums_start(turn):
        def step(outer, sums):
            norm, curve = sums
            for inner in range(4):
                n = outer * 4 + inner
                mine = s.res[node(n), :]
                norm = norm + s.weight[pl.ds(n, 1), :] * mine * mine
                curve = curve + mine * s.app[node(n), :]
            return norm, curve

        zero = jnp.zeros((m, cells), jnp.float32)
        norm, curve = lax.fori_loop(0, NB // 4, step, (zero, zero))
        total = lax.dot_general(
            jnp.ones((8, cells), jnp.float32),
            jnp.concatenate([norm, curve], 0),
            (((1,), (1,)), ((), ())),
            precision=HIGHEST,
            preferred_element_type=jnp.float32,
        )
        s.ps[turn] = total[0:1, :]
        copies = [
            remote(
                s.ps.at[turn], s.pr.at[turn, k], s.s_sum, (turn, k),
                {"ex": shifted("ex", a), "ey": shifted("ey", b)},
            )
            for k, (a, b) in enumerate(around)
        ]
        for copy in copies:
            copy.start()
        return copies

    def sums_end(turn, copies):
        total = s.ps[turn]
        for k, copy in enumerate(copies):
            copy.wait_recv()
            total = total + s.pr[turn, k]
        for copy in copies:
            copy.wait_send()
        row = lax.broadcasted_iota(jnp.int32, (m, 2 * m), 0)
        column = lax.broadcasted_iota(jnp.int32, (m, 2 * m), 1)
        pick = lambda offset: jnp.sum(
            jnp.where(column == row + offset, total, 0.0), axis=1, keepdims=True
        )
        return pick(0), pick(m)

    for g, c, copy in first:
        copy.wait_recv()

        arrived = planes_of(s.rbuf.at[g - 1, c], mc)
        for n in range(NB):
            rows = pl.ds(n * mp + c * mc, mc)
            s.res[rows, :] = s.res[rows, :] + spread(arrived, n, mc, False)

    def add_far(piece):
        def one_node(i):
            n = bounds[piece] + i
            rows = tile((NB + n) * gp, gm)
            total = s.spec[rows, :]
            for g in hops:
                total = total + dot(s.fwd[g], pile(s.fo[g - 1, n]))
            s.spec[rows, :] = total

        arrive(second[piece])
        loop(bounds[piece + 1] - bounds[piece], 7, one_node)

    assemble(s.res, 0, lambda: add_far(0))

    carry = None
    for turn in range(ITERS):
        operator()
        copies = sums_start(turn)
        if turn < ITERS - 1:
            assemble(s.app, turn + 1, (lambda: add_far(1)) if turn else (lambda: None))
        else:
            add_far(2)
        norm, curve = sums_end(turn, copies)
        if turn == 0:
            step_size = norm / curve
        else:
            ratio = norm / carry[0]
            step_size = norm / (curve - ratio * norm / carry[1])
        carry = norm, step_size

        def update(n, turn=turn):
            rows = node(n)
            search, along = s.res[rows, :], s.app[rows, :]
            residual = search
            if turn:
                search = search + ratio * s.dir[rows, :]
                s.x[rows, :] = s.x[rows, :] + step_size * search
            else:
                s.x[rows, :] = step_size * search
            if turn < ITERS - 1:
                if turn:
                    along = along + ratio * s.along[rows, :]
                s.dir[rows, :] = search
                s.along[rows, :] = along
                s.res[rows, :] = residual - step_size * along

        loop(NB, 4, update)

    def solved(c):
        return lambda n: s.x[n * mp + c * mo : n * mp + (c + 1) * mo, :]

    third = []
    for c in range(p.parts):

        def put(k, value, c=c):
            s.xsend[c, k * mo : (k + 1) * mo, :] = value

        pick_planes(solved(c), put, mo)
        for g in hops:
            copy = remote(
                s.xsend.at[c], s.xr.at[g - 1, c], s.s_b1, (g - 1, c),
                {"fourier": shifted("fourier", g)},
            )
            copy.start()
            third.append((g, c, copy))

    for copies in couple + inner_parts + second:
        for copy in copies:
            copy.wait_send()
    for _, _, copy in first:
        copy.wait_send()

    for piece in range(3, len(second)):
        add_far(piece)
    inverse_coef = 1.0 / s.coef[...]

    def restore(g, c, load):
        per = LANES // mo
        for block in range(NB // per):
            nodes = range(block * per, (block + 1) * per)
            rows = permuted(jnp.concatenate([load(n) for n in nodes], 0), s.oneT)
            for k, n in enumerate(nodes):
                piece = rows[k * mo : (k + 1) * mo]
                s.xe[n * op : n * op + mo, :] = piece
                start_row = n * gp + g * m + c * mo
                s.spec[start_row : start_row + mo, :] = piece

    def from_inner(j):
        inner = s.spec[pl.ds(NB * gp + j, DEEP, stride=gp), :]
        matrix = s.invf[tile(j * TALL, TALL), :DEEP]
        return product(matrix, inner) * inverse_coef

    def from_cycle(j, k):
        matrix = s.ct[tile(j * DEEP, TALL), :NB]
        return product(matrix, s.xe[pl.ds(k, NB, stride=op), :])

    def inner_rows(j):
        return pl.ds(NB * gp + j, NI, stride=gp)

    for c in range(p.parts):
        restore(0, c, solved(c))

        def own_mode(k, c=c):
            j = c * mo + k
            s.spec[inner_rows(j), :] = (from_inner(j) - from_cycle(j, k))[:NI]

        loop(mo, 8, own_mode)

    def own_velocity(n):
        out[n] = dot(s.back[...], pile(s.spec[tile(n * gp, m), :]))

    loop(NODES, 9, own_velocity)

    def base(k):
        s.spec[inner_rows(m + k), :] = from_inner(m + k)[:NI]

    loop(gm - m, 8, base)

    for g, c, copy in third:
        copy.wait_recv()
        arrived = planes_of(s.xr.at[g - 1, c], mo)
        restore(g, c, lambda n, arrived=arrived: spread(arrived, n, mo, True))

        def far_mode(k, g=g, c=c):
            j = g * m + c * mo + k
            s.spec[inner_rows(j), :] = s.spec[inner_rows(j), :] - from_cycle(j, k)[:NI]

        loop(mo, 8, far_mode)

        def far_velocity(n, g=g, c=c):
            rows = s.spec[tile(n * gp + g * m + c * mo, mo), :]
            out[n] = out[n] + dot(s.far[(g - 1) * p.parts + c], pile(rows))

        loop(NODES, 9, far_velocity)

    for _, _, copy in third:
        copy.wait_send()


def on_device(forcing, element_coef, schur, couple, inner_inv, element_cell):
    planes, _, elements = forcing.shape
    modes = schur.shape[0]
    sizes = tuple(lax.axis_size(axis) for axis in ("fourier", "ex", "ey"))
    p = Plan(sizes, modes, planes)
    me = lax.axis_index("fourier")
    length = planes * p.groups

    def ordered(dim, size):
        place = lax.broadcasted_iota(jnp.int32, (length, length), dim)
        return lax.rem(me + p.groups - place // size, p.groups) * size + place % size

    table = dft_values(ordered(0, modes), ordered(1, planes), length)
    pinned = lambda value: pltpu.with_memory_space_constraint(value, pltpu.HBM)
    scratch = layout(p)
    whole = pl.BlockSpec(memory_space=pltpu.VMEM)
    stay = pl.BlockSpec(memory_space=pltpu.HBM)
    velocity = pl.pallas_call(
        functools.partial(kernel, p, tuple(scratch)),
        out_shape=jax.ShapeDtypeStruct((NODES, planes, elements), jnp.float32),
        in_specs=[stay] * 6 + [whole],
        out_specs=whole,
        scratch_shapes=list(scratch.values()),
        compiler_params=pltpu.CompilerParams(
            collective_id=0, has_side_effects=True, vmem_limit_bytes=44 << 20
        ),
        cost_estimate=pl.CostEstimate(flops=10**9, bytes_accessed=2 * 10**8, transcendentals=0),
    )(
        pinned(jnp.transpose(forcing, (1, 0, 2))),
        pinned(element_coef[None]),
        pinned(element_cell[None]),
        pinned(jnp.transpose(schur, (1, 2, 0))),
        pinned(jnp.transpose(couple, (2, 1, 0))),
        pinned(jnp.transpose(inner_inv, (1, 2, 0))),
        table,
    )
    return jnp.transpose(velocity, (1, 0, 2))


def solution(mesh):
    placed = (
        P("fourier", None, ("ex", "ey")),
        P(("ex", "ey")),
        P("fourier", None, None),
        P("fourier", None, None),
        P("fourier", None, None),
        P(("ex", "ey")),
    )
    return jax.shard_map(
        on_device,
        mesh=mesh,
        in_specs=placed,
        out_specs=P("fourier", None, ("ex", "ey")),
        check_vma=False,
    )
```

```python
import functools
import math
import types

import jax
import jax.numpy as jnp
from jax import lax
from jax.experimental import pallas as pl
from jax.experimental.pallas import tpu as pltpu
from jax.sharding import PartitionSpec as P

P_SIZE = 8
ITERS = 3
ELX = 8
ELY = 16
NB = 4 * P_SIZE
NI = (P_SIZE - 1) ** 2
NODES = NB + NI
DEEP = 64
TALL = 64
LANES = 128
WIDE = 256
PLANES = 2 * P_SIZE + 1
HIGHEST = lax.Precision.HIGHEST


def dft_values(row_index, plane_index, length):
    plane_pos = plane_index.astype(jnp.float32)
    waves = ((row_index + 1) // 2).astype(jnp.float32)
    angles = 2.0 * math.pi * waves * plane_pos / length
    factor = math.sqrt(2.0 / length)
    result = jnp.where(row_index % 2 == 1, factor * jnp.cos(angles), factor * jnp.sin(angles))
    result = jnp.where(row_index == 0, 1.0 / math.sqrt(length), result)
    return jnp.where(
        row_index == length - 1, jnp.cos(math.pi * plane_pos) / math.sqrt(length), result
    )


def stacked(values):
    high = values.astype(jnp.bfloat16).astype(jnp.float32)
    return jnp.concatenate([high, high, values - high], 1).astype(jnp.bfloat16)


def split(value):
    high = value.astype(jnp.bfloat16)
    return high, (value - high.astype(jnp.float32)).astype(jnp.bfloat16)


def dot(a, b):
    return jnp.dot(a, b, preferred_element_type=jnp.float32)


def product(a, b):
    (ah, al), (bh, bl) = split(a), split(b)
    rows = a.shape[0]
    both = dot(jnp.concatenate([ah, al], 0), bh)
    return both[:rows] + (both[rows:] + dot(ah, bl))


def pile(value):
    high, low = split(value)
    return jnp.concatenate([high, low, high], 0)


def apply_table(table, values):
    result = dot(table, jnp.concatenate([pile(value) for value in values], 1))
    return [result[:, k * LANES : (k + 1) * LANES] for k in range(len(values))]


def pairs(start, stop, unroll, body):
    count = (stop - start) // 2
    loop(count, unroll, lambda i: body([start + 2 * i, start + 2 * i + 1]))
    if (stop - start) % 2:
        body([stop - 1])


def aligned(start, size):
    return pl.ds(start if isinstance(start, int) else pl.multiple_of(start, size), size)


def tile(start, size):
    return pl.ds(start if isinstance(start, int) else pl.multiple_of(start, 8), size)


def loop(count, unroll, body):
    while count % unroll:
        unroll -= 1

    def step(outer, carry):
        for inner in range(unroll):
            body(outer * unroll + inner)
        return carry

    lax.fori_loop(0, count // unroll, step, 0)


class Plan:
    def __init__(self, sizes, modes, planes):
        self.groups, self.ex, self.ey = sizes
        self.modes, self.planes = modes, planes
        self.all_modes = self.groups * modes
        self.chunk = min(16, modes)
        self.chunks = modes // self.chunk
        self.part = min(32, modes)
        self.parts = modes // self.part
        self.fold = max(1, LANES // modes)
        self.couple_rows = NB // self.fold
        self.couple_bits = 2
        while self.ey % 2**self.couple_bits:
            self.couple_bits -= 1
        self.couple_ways = 2**self.couple_bits
        step = 8 * self.couple_ways
        self.couple_part = -(-NI * self.couple_rows // step) * 8
        self.couple_all = max(DEEP * self.couple_rows, self.couple_part * self.couple_ways)
        self.inner_rows = -(-NI // self.fold)
        self.inner_ways = self.ex * self.ey
        self.inner_part = -(-self.inner_rows * TALL // (8 * self.inner_ways)) * 8
        self.inner_all = self.inner_part * self.inner_ways
        self.peers = self.ex * self.ey - 1
        self.pitch = modes + 8
        self.all_pitch = self.all_modes + 8
        self.chunk_pitch = self.chunk + 8
        self.matrix = NB + 8


def layout(p):
    f32 = lambda *dims: pltpu.VMEM(dims, jnp.float32)
    half = lambda *dims: pltpu.VMEM(dims, jnp.bfloat16)
    dma = lambda *dims: pltpu.SemaphoreType.DMA(dims)
    far, m, z = p.groups - 1, p.modes, p.planes
    field = f32(NB * p.pitch, LANES)
    return dict(
        f=f32(NODES, z, LANES),
        fo=f32(far, NI, z, LANES),
        spec=f32((NB + DEEP) * p.all_pitch, LANES),
        res=field,
        app=field,
        x=field,
        dir=field,
        along=field,
        cin=f32(NI, NB, m),
        sin=f32(NB, NB, m),
        iin=f32(NI, NI, m),
        cpack=f32(p.groups, p.couple_all, LANES),
        ipack=f32(p.groups, p.inner_all, LANES),
        cf=f32(p.all_modes * p.matrix, LANES),
        invf=f32(p.all_modes * TALL, LANES),
        sch=f32(m * p.matrix, LANES),
        cbuf=f32(NB * p.chunk_pitch, LANES),
        cgrid=f32(NB * p.chunk, LANES),
        sbuf=f32(far, p.chunks, PLANES * p.chunk, LANES),
        rbuf=f32(far, p.chunks, PLANES * p.chunk, LANES),
        xsend=f32(p.parts, PLANES * p.part, LANES),
        xr=f32(far, p.parts, PLANES * p.part, LANES),
        fwd=half(p.groups, p.all_modes, 3 * z),
        back=half(z, 3 * m),
        far=half(far * p.parts, z, 3 * p.part),
        one=half(LANES, LANES),
        oneT=half(LANES, LANES),
        scale=f32(8, LANES),
        coef=f32(1, LANES),
        cell=pltpu.VMEM((1, LANES), jnp.int32),
        keep=f32(NB, LANES),
        weight=f32(NB, LANES),
        xs=f32(ITERS, 2, 2, m, LANES),
        xh=f32(ITERS, 2, 2, m, LANES),
        ys=f32(ITERS, 2, m, LANES),
        yh=f32(ITERS, 3, 2, m, LANES),
        ps=f32(ITERS, p.peers, 1, 2 * m),
        pr=f32(ITERS, p.peers, 1, 2 * m),
        s_local=dma(7),
        s_halo=dma(2, ITERS, 8),
        s_sum=dma(2, ITERS),
        s_couple=dma(2, 1 + p.couple_bits, far, 1),
        s_inner=dma(2, 3, far, max(1, p.ex - 1, p.ey - 1)),
        s_f1=dma(2, far, p.chunks),
        s_f2=dma(2, far, 4),
        s_b1=dma(2, far, p.parts),
    )


def kernel(p, names, forcing, coef_in, cell_in, schur_in, couple_in, inner_in, table, out, *refs):
    s = types.SimpleNamespace(**dict(zip(names, refs)))
    m, z, gm, mc = p.modes, p.planes, p.all_modes, p.chunk
    mp, gp, cp, nb = p.pitch, p.all_pitch, p.chunk_pitch, p.matrix
    mo = p.part
    cells = LANES
    sizes = {"fourier": p.groups, "ex": p.ex, "ey": p.ey}
    place = {axis: lax.axis_index(axis) for axis in sizes}
    lane = lax.broadcasted_iota(jnp.int32, (m, cells), 1)
    lane_row = lane // ELY
    lane_col = lane % ELY

    def shifted(axis, by):
        return lax.rem(place[axis] + (by % sizes[axis]), sizes[axis])

    def remote(source, target, sems, index, device):
        return pltpu.make_async_remote_copy(
            src_ref=source,
            dst_ref=target,
            send_sem=sems.at[(0,) + index],
            recv_sem=sems.at[(1,) + index],
            device_id=device,
            device_id_type=pl.DeviceIdType.MESH,
        )

    hops = range(1, p.groups)
    around = [(a, b) for a in range(p.ex) for b in range(p.ey) if a or b]

    bottom = lambda k: k
    top = lambda k: 3 * P_SIZE - k
    left = lambda k: (NB - k) % NB
    right = lambda k: P_SIZE + k
    last = cells - ELY

    def turned(value, shift):
        shift = shift % cells
        return pltpu.roll(value, shift, 1) if shift else value

    def grid(rows):
        where = lax.broadcasted_iota(jnp.int32, (rows, cells), 1)
        return where // ELY, where % ELY

    def compress(load, store, rows):
        row, col = grid(rows)

        def sideways(k):
            return load(left(k)) + jnp.where(row == 0, 0.0, turned(load(right(k)), ELY))

        corner = sideways(P_SIZE)
        store(0, sideways(0) + jnp.where(col == 0, 0.0, turned(corner, 1)))
        for k in range(1, P_SIZE):
            store(k, load(k) + jnp.where(col == 0, 0.0, turned(load(top(k)), 1)))
            store(P_SIZE - 1 + k, sideways(k))
        edge = load(right(0)) + jnp.where(col == 0, 0.0, turned(load(right(P_SIZE)), 1))
        far_row = turned(edge, -last)
        far_col = turned(corner, 1 - ELY)
        for k in range(1, P_SIZE):
            far_row = jnp.where(row == k, turned(load(right(k)), ELY * k - last), far_row)
            far_col = jnp.where(col == k, turned(load(top(k)), k - ELY + 1), far_col)
        tip = turned(load(top(P_SIZE)), P_SIZE - ELY + 1)
        store(2 * P_SIZE - 1, far_row)
        store(
            2 * P_SIZE,
            jnp.where(
                col < P_SIZE,
                far_col,
                jnp.where((col == P_SIZE) & (row == ELX - 1), tip, 0.0),
            ),
        )

    def pick_planes(load, store, rows):
        row, col = grid(rows)
        far_row = turned(load(right(0)), -last)
        far_col = turned(load(top(0)), 1 - ELY)
        for k in range(P_SIZE):
            store(k, load(k))
        for k in range(1, P_SIZE):
            store(P_SIZE - 1 + k, load(left(k)))
            far_row = jnp.where(row == k, turned(load(right(k)), ELY * k - last), far_row)
        for k in range(1, P_SIZE + 1):
            far_col = jnp.where(col == k, turned(load(top(k)), k - ELY + 1), far_col)
        store(2 * P_SIZE - 1, far_row)
        store(2 * P_SIZE, far_col)

    def spread(load, n, rows, inside):
        row, col = grid(rows)
        if n < P_SIZE:
            return load(n)
        if n > 3 * P_SIZE:
            return load(P_SIZE - 1 + NB - n)
        if n < 2 * P_SIZE:
            k = n - P_SIZE
            beside = turned(load(k and P_SIZE - 1 + k), -ELY) if inside else 0.0
            return jnp.where(
                row == ELX - 1, turned(load(2 * P_SIZE - 1), last - ELY * k), beside
            )
        k = 3 * P_SIZE - n
        if inside:
            above = turned(load(k) if k < P_SIZE else spread(load, P_SIZE, rows, True), -1)
        else:
            above = 0.0
        return jnp.where(col == ELY - 1, turned(load(2 * P_SIZE), ELY - 1 - k), above)

    def planes_of(ref, rows):
        return lambda k: ref[k * rows : (k + 1) * rows, :]

    loads = [
        pltpu.make_async_copy(couple_in, s.cin, s.s_local.at[0]),
        pltpu.make_async_copy(inner_in, s.iin, s.s_local.at[1]),
        pltpu.make_async_copy(
            forcing.at[pl.ds(NB, NI)], s.f.at[pl.ds(NB, NI)], s.s_local.at[2]
        ),
        pltpu.make_async_copy(forcing.at[pl.ds(0, NB)], s.f.at[pl.ds(0, NB)], s.s_local.at[3]),
        pltpu.make_async_copy(schur_in, s.sin, s.s_local.at[4]),
        pltpu.make_async_copy(coef_in, s.coef, s.s_local.at[5]),
        pltpu.make_async_copy(cell_in, s.cell, s.s_local.at[6]),
    ]
    for k in (0, 2, 3, 5, 6, 1, 4):
        loads[k].start()

    s.xh[...] = jnp.zeros_like(s.xh)
    s.yh[...] = jnp.zeros_like(s.yh)

    barrier = pltpu.get_barrier_semaphore()
    for a, b in around:
        pl.semaphore_signal(
            barrier,
            inc=1,
            device_id={"ex": shifted("ex", a), "ey": shifted("ey", b)},
            device_id_type=pl.DeviceIdType.MESH,
        )
    for hop in hops:
        pl.semaphore_signal(
            barrier,
            inc=1,
            device_id={"fourier": shifted("fourier", hop)},
            device_id_type=pl.DeviceIdType.MESH,
        )

    def clear(ref, start, stop):
        if stop > start:
            ref[pl.ds(start, stop - start), :] = jnp.zeros((stop - start, LANES), jnp.float32)

    for g in range(p.groups):
        s.fwd[g] = stacked(table[:, g * z : (g + 1) * z])

    br = p.couple_rows
    own_rows = NI * br
    got_rows = p.couple_part * p.couple_ways
    clear(s.cpack.at[0], own_rows, p.couple_all)
    for g in hops:
        clear(s.cpack.at[g], got_rows, p.couple_all)
    loads[0].wait()
    for i in range(NI):
        s.cpack[0, i * br : (i + 1) * br, :] = jnp.concatenate(
            [s.cin[i, k * br : (k + 1) * br, :] for k in range(p.fold)], 1
        )
    pl.semaphore_wait(barrier, len(around) + p.groups - 1)

    def share_by_halves(pack, part, sems):
        stages, bits = [], p.couple_bits
        digit = [place["ey"] // 2**k % 2 for k in range(bits)]
        turn = sum(digit[k] * 2 ** (bits - 1 - k) for k in range(bits))
        for stage in range(bits + 1):
            held = 2 ** max(0, stage - 1)
            rows = tile(turn // held * (held * part), held * part)
            if stage:
                flip = 2 ** (bits - stage)
                other = {"ey": place["ey"] + flip * (1 - 2 * digit[bits - stage])}
            stages.append(
                [
                    remote(
                        pack.at[g if stage else 0, rows], pack.at[g, rows], sems,
                        (stage, g - 1, 0),
                        other if stage else {"fourier": shifted("fourier", g)},
                    )
                    for g in hops
                ]
            )
        return stages

    def share_out(pack, part, sems):
        turn = place["ey"] * p.ex + place["ex"]
        rows = tile(turn * part, part)
        stages = [
            [
                remote(
                    pack.at[0, rows], pack.at[g, rows], sems, (0, g - 1, 0),
                    {"fourier": shifted("fourier", g)},
                )
                for g in hops
            ]
        ]
        for axis in ("ex", "ey"):
            if axis == "ey":
                rows = tile(place["ey"] * p.ex * part, p.ex * part)
            stages.append(
                [
                    remote(
                        pack.at[g, rows], pack.at[g, rows], sems, (len(stages), g - 1, k - 1),
                        {axis: shifted(axis, k)},
                    )
                    for g in hops
                    for k in range(1, sizes[axis])
                ]
            )
        return stages

    def start(stage):
        for copy in stage:
            copy.start()

    def arrive(stage):
        for copy in stage:
            copy.wait_recv()

    couple = share_by_halves(s.cpack, p.couple_part, s.s_couple)
    inner_parts = share_out(s.ipack, p.inner_part, s.s_inner)
    start(couple[0])

    bounds = [0, 8, 22, 36, NI]
    second = [
        [
            remote(
                forcing.at[pl.ds(NB + a, b - a)], s.fo.at[g - 1, pl.ds(a, b - a)], s.s_f2,
                (g - 1, k), {"fourier": shifted("fourier", g)},
            )
            for g in hops
        ]
        for k, (a, b) in enumerate(zip(bounds, bounds[1:]))
    ]
    start(second[0])

    def flat(pack, g, start, count, stride, width):
        rows = pack[g, pl.ds(start, count, stride=stride) if stride > 1 else pl.ds(start, count), :]
        if count < LANES:
            rows = jnp.concatenate([rows, jnp.zeros((LANES - count, LANES), jnp.float32)], 0)
        return jnp.transpose(rows)

    def couple_matrices(g):
        for b in range(br):
            turned_rows = flat(s.cpack, g, b, DEEP, br, NI)
            for k in range(p.fold):
                s.cf[pl.ds(g * m * nb + k * br + b, m, stride=nb), :] = turned_rows[
                    k * m : (k + 1) * m
                ]

    def inner_matrices(g):
        for i in range(ir):
            turned_rows = flat(s.ipack, g, i * TALL, TALL, 1, NI)
            for k in range(p.fold):
                if k * ir + i < TALL:
                    s.invf[pl.ds(g * m * TALL + k * ir + i, m, stride=TALL), :] = turned_rows[
                        k * m : (k + 1) * m
                    ]

    def spectrum(nodes):
        values = apply_table(s.fwd[0], [s.f[n] for n in nodes])
        for n, value in zip(nodes, values):
            s.spec[tile(n * gp, gm), :] = value

    clear(s.spec, NODES * gp, (NB + DEEP) * gp)
    loads[2].wait()
    pairs(NB, NODES, 4, spectrum)
    loads[3].wait()
    pairs(0, NB, 4, spectrum)
    couple_matrices(0)

    loads[5].wait()
    loads[6].wait()
    lines = lax.broadcasted_iota(jnp.int32, (LANES, LANES), 0)
    hot = jnp.where(lines == s.cell[...], 1.0, 0.0).astype(jnp.float32)
    hot_t = jnp.transpose(hot)
    s.oneT[...] = hot.astype(jnp.bfloat16)
    s.one[...] = hot_t.astype(jnp.bfloat16)
    s.scale[...] = lax.dot_general(
        jnp.broadcast_to(s.coef[...], (8, LANES)),
        hot_t,
        (((1,), (0,)), ((), ())),
        precision=HIGHEST,
        preferred_element_type=jnp.float32,
    )

    def permuted(rows, hot_ref):
        both = dot(jnp.concatenate(split(rows), 0), hot_ref[...])
        return both[: rows.shape[0]] + both[rows.shape[0] :]

    def condense(g, c, store):
        def one_mode(k):
            j = g * m + c * mc + k
            inner = s.spec[pl.ds(NB * gp + j, DEEP, stride=gp), :]
            matrix = s.cf[tile(j * nb, NB), :DEEP]
            s.cbuf[pl.ds(k, NB, stride=cp), :] = s.spec[
                pl.ds(j, NB, stride=gp), :
            ] - product(matrix, inner)

        loop(mc, 16, one_mode)
        per = WIDE // mc
        for block in range(NB // per):
            rows = [s.cbuf[n * cp : n * cp + mc, :] for n in range(block * per, (block + 1) * per)]
            store(block, permuted(jnp.concatenate(rows, 0), s.one))

    def keep_own(c):
        per = WIDE // mc

        def store(block, rows):
            for k in range(per):
                n = block * per + k
                s.res[n * mp + c * mc : n * mp + (c + 1) * mc, :] = rows[k * mc : (k + 1) * mc]

        return store

    own_chunks = list(range(p.chunks))

    def condense_own():
        if own_chunks:
            c = own_chunks.pop(0)
            condense(0, c, keep_own(c))

    arrive(couple[0])
    for copies in couple[1:2]:
        start(copies)
    condense_own()
    loads[1].wait()
    ir = p.inner_rows
    clear(s.ipack.at[0], 0, p.inner_all)
    for i in range(ir):
        picks = [s.iin[min(k * ir + i, NI - 1), :, :] for k in range(p.fold)]
        s.ipack[0, i * TALL : i * TALL + NI, :] = jnp.concatenate(picks, 1)
    start(inner_parts[0])

    for stage, copies in enumerate(couple[2:]):
        if stage == 0:
            condense_own()
        arrive(couple[stage + 1])
        start(copies)
    condense_own()
    arrive(inner_parts[0])
    start(inner_parts[1])
    arrive(couple[-1])

    first = []
    for g in hops:
        couple_matrices(g)
        for c in range(p.chunks):

            def store(block, rows):
                s.cgrid[block * WIDE : (block + 1) * WIDE, :] = rows

            condense(g, c, store)

            def put(k, value, g=g, c=c):
                s.sbuf[g - 1, c, k * mc : (k + 1) * mc, :] = value

            compress(planes_of(s.cgrid, mc), put, mc)
            copy = remote(
                s.sbuf.at[g - 1, c], s.rbuf.at[g - 1, c], s.s_f1, (g - 1, c),
                {"fourier": shifted("fourier", -g)},
            )
            copy.start()
            first.append((g, c, copy))

    for stage in second[1:]:
        start(stage)
    arrive(inner_parts[1])
    start(inner_parts[2])

    while own_chunks:
        condense_own()

    flipped = jnp.transpose(table[...])[:z]
    s.back[...] = stacked(flipped[:, :m])
    for k in range((p.groups - 1) * p.parts):
        s.far[k] = stacked(flipped[:, m + k * mo : m + (k + 1) * mo])

    loads[4].wait()
    group = LANES // NB
    for q in range(NB // group):
        rows = jnp.concatenate([s.sin[q * group + k] for k in range(group)], 0)
        if m < LANES:
            rows = jnp.concatenate([rows, jnp.zeros((LANES, LANES - m), jnp.float32)], 1)
        square = jnp.transpose(rows)[:m]
        high = square.astype(jnp.bfloat16).astype(jnp.float32)
        low = square - high
        where = lax.broadcasted_iota(jnp.int32, (m, LANES), 1)
        for k in range(group):
            first_half = jnp.where(where < NB, turned(high, -k * NB), turned(high, NB - k * NB))
            s.sch[pl.ds(q * group + k, m, stride=nb), :] = jnp.where(
                where < 2 * NB, first_half, turned(low, 2 * NB - k * NB)
            )

    slots = lax.broadcasted_iota(jnp.int32, (NB, cells), 0)
    places = lax.broadcasted_iota(jnp.int32, (NB, cells), 1)
    row_ids = place["ex"] * ELX + places // ELY
    col_ids = place["ey"] * ELY + places % ELY
    dropped = (
        ((slots == 0) | (slots >= 3 * P_SIZE)) & (row_ids == 0)
        | (slots >= P_SIZE) & (slots <= 2 * P_SIZE) & (row_ids == ELX * p.ex - 1)
        | (slots <= P_SIZE) & (col_ids == 0)
        | (slots >= 2 * P_SIZE) & (slots <= 3 * P_SIZE) & (col_ids == ELY * p.ey - 1)
    )
    keep = jnp.where(dropped, 0.0, 1.0).astype(jnp.float32)
    s.keep[...] = keep
    s.weight[...] = keep * jnp.where(slots % P_SIZE == 0, 0.25, 0.5)

    def couple_beside(q):
        group = LANES // NB
        rows = [s.cf[tile((q * group + k) * nb, NB), :] for k in range(group)]
        square = jnp.transpose(jnp.concatenate(rows, 0))[:TALL]
        where = lax.broadcasted_iota(jnp.int32, (TALL, LANES), 1)
        for k in range(group):
            place_rows = tile((q * group + k) * TALL, TALL)
            s.invf[place_rows, :] = jnp.where(
                (where >= DEEP) & (where < DEEP + NB),
                -turned(square, DEEP - k * NB),
                s.invf[place_rows, :],
            )

    inner_matrices(0)

    def far_matrices():
        arrive(inner_parts[2])
        for g in hops:
            inner_matrices(g)

    fillers = [far_matrices, lambda: loop(gm * NB // LANES, 4, couple_beside)]

    def node(n):
        return tile(n * mp, m)

    def exists(axis, step):
        if step == 0:
            return None
        return place[axis] < sizes[axis] - 1 if step > 0 else place[axis] > 0

    def guarded(ex_step, ey_step, action):
        tests = [t for t in (exists("ex", ex_step), exists("ey", ey_step)) if t is not None]
        pl.when(functools.reduce(jnp.logical_and, tests))(action)

    def halo_copy(turn, number, source, target, ex_step, ey_step):
        copy = pltpu.make_async_remote_copy(
            src_ref=source,
            dst_ref=target,
            send_sem=s.s_halo.at[0, turn, number],
            recv_sem=s.s_halo.at[1, turn, number],
            device_id={"ex": shifted("ex", ex_step), "ey": shifted("ey", ey_step)},
            device_id_type=pl.DeviceIdType.MESH,
        )
        guarded(ex_step, ey_step, copy.start)
        return (
            lambda: guarded(-ex_step, -ey_step, copy.wait_recv),
            lambda: guarded(ex_step, ey_step, copy.wait_send),
        )

    def assemble(ref, turn, meanwhile):
        copies = []
        up = down = None
        for k in range(P_SIZE + 1):
            ends = jnp.where(lane_col == ELY - 1, ref[node(top(k)), :], ref[node(bottom(k)), :])
            ends = turned(ends, k)
            up = ends if k == 0 else jnp.where(lane_col == k - 1, ends, up)
            down = ends if k == 0 else jnp.where(lane_col == k, ends, down)
        up = jnp.where(lane_col <= P_SIZE, turned(up, 1 - ELY), 0.0)
        down = jnp.where(lane_col <= P_SIZE, down, 0.0)
        s.ys[turn, 0] = up
        s.ys[turn, 1] = down
        for slot, ex_step in ((1, 1), (2, -1), (0, 0)):
            for way, ey_step in ((0, 1), (1, -1)):
                copies.append(
                    halo_copy(
                        turn, 2 * slot + way, s.ys.at[turn, way], s.yh.at[turn, slot, way],
                        ex_step, ey_step,
                    )
                )
        for k in range(P_SIZE):
            ends = jnp.where(lane_row == ELX - 1, ref[node(right(k)), :], ref[node(left(k)), :])
            ends = turned(ends, ELY * k)
            up = ends if k == 0 else jnp.where(lane_row == k - 1, ends, up)
            down = ends if k == 0 else jnp.where(lane_row == k, ends, down)
        up = turned(up, -last)
        s.xs[turn, 0, 0] = up
        s.xs[turn, 1, 0] = down
        s.xs[turn, 0, 1] = turned(ref[node(right(P_SIZE)), :], -last)
        s.xs[turn, 1, 1] = ref[node(left(P_SIZE)), :]
        for way, ex_step in ((0, 1), (1, -1)):
            copies.append(
                halo_copy(turn, 6 + way, s.xs.at[turn, way], s.xh.at[turn, way], ex_step, 0)
            )

        for k in range(P_SIZE + 1):
            here_left, here_right = ref[node(left(k)), :], ref[node(right(k)), :]
            ref[node(left(k)), :] = here_left + jnp.where(
                lane_row == 0, 0.0, turned(here_right, ELY)
            )
            ref[node(right(k)), :] = here_right + jnp.where(
                lane_row == ELX - 1, 0.0, turned(here_left, -ELY)
            )
        meanwhile()
        for wait, _ in copies:
            wait()

        for k in range(P_SIZE + 1):
            part, lanes = divmod(k, P_SIZE)
            if part:
                low = s.xh[turn, 0, part]
                high = turned(s.xh[turn, 1, part], last)
            else:
                if k == 0:
                    from_low, from_high = s.xh[turn, 0, 0], turned(s.xh[turn, 1, 0], last)
                low = turned(jnp.where(lane_row == k, from_low, from_high), -ELY * k)
                high = low
            for n, halo, row in ((left(k), low, 0), (right(k), high, ELX - 1)):
                value = ref[node(n), :] + jnp.where(lane_row == row, halo, 0.0)
                if n % (2 * P_SIZE) > P_SIZE:
                    value = value * s.keep[n : n + 1, :]
                ref[node(n), :] = value

        lines = []
        for way in range(2):
            line = s.yh[turn, 0, way]
            before = jnp.where(
                lane == 0, turned(s.yh[turn, 1, way], P_SIZE), turned(line, P_SIZE)
            )
            after = jnp.where(
                lane == last + P_SIZE, turned(s.yh[turn, 2, way], -P_SIZE), turned(line, -P_SIZE)
            )
            lines.append(
                line
                + jnp.where(lane_col == 0, before, jnp.where(lane_col == P_SIZE, after, 0.0))
            )
        low_all, high_all = lines[0], turned(lines[1], ELY - 1)
        for k in range(P_SIZE + 1):
            b, t = bottom(k), top(k)
            here_bottom, here_top = ref[node(b), :], ref[node(t), :]
            ends = turned(jnp.where(lane_col == k, low_all, high_all), -k)
            ref[node(b), :] = s.keep[b : b + 1, :] * (
                here_bottom + jnp.where(lane_col == 0, ends, turned(here_top, 1))
            )
            ref[node(t), :] = s.keep[t : t + 1, :] * (
                here_top + jnp.where(lane_col == ELY - 1, ends, turned(here_bottom, -1))
            )
        for _, leave in copies:
            leave()

    def operator():
        scale = s.scale[0:1, :]

        def one_mode(k):
            value = s.res[pl.ds(k, NB, stride=mp), :]
            matrix = s.sch[tile(k * nb, NB), : 3 * NB].astype(jnp.bfloat16)
            s.app[pl.ds(k, NB, stride=mp), :] = dot(matrix, pile(value)) * scale

        loop(m, 8, one_mode)

    def sums_start(turn):
        def step(outer, sums):
            norm, curve = sums
            for inner in range(4):
                n = outer * 4 + inner
                mine = s.res[node(n), :]
                norm = norm + s.weight[pl.ds(n, 1), :] * mine * mine
                curve = curve + mine * s.app[node(n), :]
            return norm, curve

        zero = jnp.zeros((m, cells), jnp.float32)
        norm, curve = lax.fori_loop(0, NB // 4, step, (zero, zero))
        total = lax.dot_general(
            jnp.ones((8, cells), jnp.float32),
            jnp.concatenate([norm, curve], 0),
            (((1,), (1,)), ((), ())),
            precision=HIGHEST,
            preferred_element_type=jnp.float32,
        )
        for k in range(p.peers):
            s.ps[turn, k] = total[0:1, :]
        copies = [
            remote(
                s.ps.at[turn, k], s.pr.at[turn, k], s.s_sum, (turn,),
                {"ex": shifted("ex", a), "ey": shifted("ey", b)},
            )
            for k, (a, b) in enumerate(around)
        ]
        for copy in copies:
            copy.start()
        return copies

    def sums_end(turn, copies):
        whole = remote(
            s.ps.at[turn], s.pr.at[turn], s.s_sum, (turn,),
            {"ex": shifted("ex", around[0][0]), "ey": shifted("ey", around[0][1])},
        )
        whole.wait_recv()
        total = s.ps[turn, 0]
        for k in range(p.peers):
            total = total + s.pr[turn, k]
        whole.wait_send()
        row = lax.broadcasted_iota(jnp.int32, (m, 2 * m), 0)
        column = lax.broadcasted_iota(jnp.int32, (m, 2 * m), 1)
        pick = lambda offset: jnp.sum(
            jnp.where(column == row + offset, total, 0.0), axis=1, keepdims=True
        )
        return pick(0), pick(m)

    for g, c, copy in first:
        copy.wait_recv()

        arrived = planes_of(s.rbuf.at[g - 1, c], mc)
        for n in range(NB):
            rows = pl.ds(n * mp + c * mc, mc)
            s.res[rows, :] = s.res[rows, :] + spread(arrived, n, mc, False)

    def add_far(piece):
        def some_nodes(nodes):
            totals = [s.spec[tile((NB + n) * gp, gm), :] for n in nodes]
            for g in hops:
                more = apply_table(s.fwd[g], [s.fo[g - 1, n] for n in nodes])
                totals = [total + value for total, value in zip(totals, more)]
            for n, total in zip(nodes, totals):
                s.spec[tile((NB + n) * gp, gm), :] = total

        arrive(second[piece])
        pairs(bounds[piece], bounds[piece + 1], 4, some_nodes)

    assemble(s.res, 0, lambda: add_far(0))

    carry = None
    for turn in range(ITERS):
        operator()
        copies = sums_start(turn)
        if turn < ITERS - 1:
            assemble(s.app, turn + 1, fillers[turn])
        else:
            add_far(1)
        norm, curve = sums_end(turn, copies)
        if turn == 0:
            step_size = norm / curve
        else:
            ratio = norm / carry[0]
            step_size = norm / (curve - ratio * norm / carry[1])
        carry = norm, step_size

        def update(n, turn=turn):
            rows = node(n)
            search, along = s.res[rows, :], s.app[rows, :]
            residual = search
            if turn:
                search = search + ratio * s.dir[rows, :]
                s.x[rows, :] = s.x[rows, :] + step_size * search
            else:
                s.x[rows, :] = step_size * search
            if turn < ITERS - 1:
                if turn:
                    along = along + ratio * s.along[rows, :]
                s.dir[rows, :] = search
                s.along[rows, :] = along
                s.res[rows, :] = residual - step_size * along

        loop(NB, 4, update)

    def solved(c):
        return lambda n: s.x[n * mp + c * mo : n * mp + (c + 1) * mo, :]

    third = []
    for c in range(p.parts):

        def put(k, value, c=c):
            s.xsend[c, k * mo : (k + 1) * mo, :] = value

        pick_planes(solved(c), put, mo)
        for g in hops:
            copy = remote(
                s.xsend.at[c], s.xr.at[g - 1, c], s.s_b1, (g - 1, c),
                {"fourier": shifted("fourier", g)},
            )
            copy.start()
            third.append((g, c, copy))

    for copies in couple + inner_parts + second:
        for copy in copies:
            copy.wait_send()
    for _, _, copy in first:
        copy.wait_send()

    for piece in range(2, len(second)):
        add_far(piece)
    inverse_coef = 1.0 / s.coef[...]

    def restore(g, c, load):
        per = WIDE // mo
        for block in range(NB // per):
            nodes = range(block * per, (block + 1) * per)
            rows = permuted(jnp.concatenate([load(n) for n in nodes], 0), s.oneT)
            for k, n in enumerate(nodes):
                start_row = n * gp + g * m + c * mo
                s.spec[start_row : start_row + mo, :] = rows[k * mo : (k + 1) * mo]

    def inner_rows(j, count):
        return pl.ds(NB * gp + j, count, stride=gp)

    def matrix(j, lanes):
        return s.invf[tile(j * TALL, TALL), lanes]

    def scaled(j):
        return s.spec[inner_rows(j, DEEP), :] * inverse_coef

    def cycle(j):
        return s.spec[pl.ds(j, NB, stride=gp), :]

    def whole_mode(j):
        both = jnp.concatenate([scaled(j), cycle(j)], 0)
        s.spec[inner_rows(j, NI), :] = product(matrix(j, pl.ds(0, DEEP + NB)), both)[:NI]

    def base(j):
        s.spec[inner_rows(j, NI), :] = product(matrix(j, pl.ds(0, DEEP)), scaled(j))[:NI]

    def correct(j):
        value = product(matrix(j, pl.ds(DEEP, NB)), cycle(j))
        s.spec[inner_rows(j, NI), :] = s.spec[inner_rows(j, NI), :] + value[:NI]

    for c in range(p.parts):
        restore(0, c, solved(c))
        loop(mo, 16, lambda k, c=c: whole_mode(c * mo + k))

    def own_velocity(nodes):
        rows = [s.spec[tile(n * gp, m), :] for n in nodes]
        for n, value in zip(nodes, apply_table(s.back[...], rows)):
            out[n] = value

    pairs(0, NODES, 4, own_velocity)

    late = gm - mo
    loop(mo, 16, lambda k: base(late + k))

    for g, c, copy in third:
        copy.wait_recv()
        arrived = planes_of(s.xr.at[g - 1, c], mo)
        restore(g, c, lambda n, arrived=arrived: spread(arrived, n, mo, True))
        first_mode = g * m + c * mo

        def far_mode(k, first_mode=first_mode):
            if first_mode == late:
                correct(first_mode + k)
            else:
                whole_mode(first_mode + k)

        loop(mo, 16, far_mode)

        def far_velocity(nodes, g=g, c=c, first_mode=first_mode):
            rows = [s.spec[tile(n * gp + first_mode, mo), :] for n in nodes]
            values = apply_table(s.far[(g - 1) * p.parts + c], rows)
            for n, value in zip(nodes, values):
                out[n] = out[n] + value

        pairs(0, NODES, 4, far_velocity)

    for _, _, copy in third:
        copy.wait_send()


def on_device(forcing, element_coef, schur, couple, inner_inv, element_cell):
    planes, _, elements = forcing.shape
    modes = schur.shape[0]
    sizes = tuple(lax.axis_size(axis) for axis in ("fourier", "ex", "ey"))
    p = Plan(sizes, modes, planes)
    me = lax.axis_index("fourier")
    length = planes * p.groups

    def ordered(dim, size):
        place = lax.broadcasted_iota(jnp.int32, (length, length), dim)
        return lax.rem(me + p.groups - place // size, p.groups) * size + place % size

    table = dft_values(ordered(0, modes), ordered(1, planes), length)
    pinned = lambda value: pltpu.with_memory_space_constraint(value, pltpu.HBM)
    scratch = layout(p)
    whole = pl.BlockSpec(memory_space=pltpu.VMEM)
    stay = pl.BlockSpec(memory_space=pltpu.HBM)
    velocity = pl.pallas_call(
        functools.partial(kernel, p, tuple(scratch)),
        out_shape=jax.ShapeDtypeStruct((NODES, planes, elements), jnp.float32),
        in_specs=[stay] * 6 + [whole],
        out_specs=whole,
        scratch_shapes=list(scratch.values()),
        compiler_params=pltpu.CompilerParams(
            collective_id=0, has_side_effects=True, vmem_limit_bytes=44 << 20
        ),
        cost_estimate=pl.CostEstimate(flops=10**9, bytes_accessed=2 * 10**8, transcendentals=0),
    )(
        pinned(jnp.transpose(forcing, (1, 0, 2))),
        pinned(element_coef[None]),
        pinned(element_cell[None]),
        pinned(jnp.transpose(schur, (1, 2, 0))),
        pinned(jnp.transpose(couple, (2, 1, 0))),
        pinned(jnp.transpose(inner_inv, (1, 2, 0))),
        table,
    )
    return jnp.transpose(velocity, (1, 0, 2))


def solution(mesh):
    placed = (
        P("fourier", None, ("ex", "ey")),
        P(("ex", "ey")),
        P("fourier", None, None),
        P("fourier", None, None),
        P("fourier", None, None),
        P(("ex", "ey")),
    )
    return jax.shard_map(
        on_device,
        mesh=mesh,
        in_specs=placed,
        out_specs=P("fourier", None, ("ex", "ey")),
        check_vma=False,
    )
```

```python
import functools
import math
import types

import jax
import jax.numpy as jnp
from jax import lax
from jax.experimental import pallas as pl
from jax.experimental.pallas import tpu as pltpu
from jax.sharding import PartitionSpec as P

P_SIZE = 8
ITERS = 3
ELX = 8
ELY = 16
NB = 4 * P_SIZE
NI = (P_SIZE - 1) ** 2
NODES = NB + NI
DEEP = 64
TALL = 64
LANES = 128
WIDE = 256
PLANES = 2 * P_SIZE + 1
HIGHEST = lax.Precision.HIGHEST


def dft_values(row_index, plane_index, length):
    plane_pos = plane_index.astype(jnp.float32)
    waves = ((row_index + 1) // 2).astype(jnp.float32)
    angles = 2.0 * math.pi * waves * plane_pos / length
    factor = math.sqrt(2.0 / length)
    result = jnp.where(row_index % 2 == 1, factor * jnp.cos(angles), factor * jnp.sin(angles))
    result = jnp.where(row_index == 0, 1.0 / math.sqrt(length), result)
    return jnp.where(
        row_index == length - 1, jnp.cos(math.pi * plane_pos) / math.sqrt(length), result
    )


def stacked(values):
    high = values.astype(jnp.bfloat16).astype(jnp.float32)
    return jnp.concatenate([high, high, values - high], 1).astype(jnp.bfloat16)


def split(value):
    high = value.astype(jnp.bfloat16)
    return high, (value - high.astype(jnp.float32)).astype(jnp.bfloat16)


def dot(a, b):
    return jnp.dot(a, b, preferred_element_type=jnp.float32)


def product(a, b):
    (ah, al), (bh, bl) = split(a), split(b)
    rows = a.shape[0]
    both = dot(jnp.concatenate([ah, al], 0), bh)
    return both[:rows] + (both[rows:] + dot(ah, bl))


def pile(value):
    high, low = split(value)
    return jnp.concatenate([high, low, high], 0)


def apply_table(table, values):
    result = dot(table, jnp.concatenate([pile(value) for value in values], 1))
    return [result[:, k * LANES : (k + 1) * LANES] for k in range(len(values))]


def pairs(start, stop, unroll, body):
    count = (stop - start) // 2
    loop(count, unroll, lambda i: body([start + 2 * i, start + 2 * i + 1]))
    if (stop - start) % 2:
        body([stop - 1])


def aligned(start, size):
    return pl.ds(start if isinstance(start, int) else pl.multiple_of(start, size), size)


def tile(start, size):
    return pl.ds(start if isinstance(start, int) else pl.multiple_of(start, 8), size)


def loop(count, unroll, body):
    while count % unroll:
        unroll -= 1

    def step(outer, carry):
        for inner in range(unroll):
            body(outer * unroll + inner)
        return carry

    lax.fori_loop(0, count // unroll, step, 0)


class Plan:
    def __init__(self, sizes, modes, planes):
        self.groups, self.ex, self.ey = sizes
        self.modes, self.planes = modes, planes
        self.all_modes = self.groups * modes
        self.chunk = min(16, modes)
        self.chunks = modes // self.chunk
        self.part = min(32, modes)
        self.parts = modes // self.part
        self.fold = max(1, LANES // modes)
        self.couple_rows = NB // self.fold
        self.couple_bits = 2
        while self.ey % 2**self.couple_bits:
            self.couple_bits -= 1
        self.couple_ways = 2**self.couple_bits
        step = 8 * self.couple_ways
        self.couple_part = -(-NI * self.couple_rows // step) * 8
        self.couple_all = max(DEEP * self.couple_rows, self.couple_part * self.couple_ways)
        self.inner_rows = -(-NI // self.fold)
        self.inner_ways = self.ex * self.ey
        self.inner_part = -(-self.inner_rows * TALL // (8 * self.inner_ways)) * 8
        self.inner_all = self.inner_part * self.inner_ways
        self.peers = self.ex * self.ey - 1
        self.pitch = modes + 8
        self.all_pitch = self.all_modes + 8
        self.chunk_pitch = self.chunk + 8
        self.matrix = NB + 8


def layout(p):
    f32 = lambda *dims: pltpu.VMEM(dims, jnp.float32)
    half = lambda *dims: pltpu.VMEM(dims, jnp.bfloat16)
    dma = lambda *dims: pltpu.SemaphoreType.DMA(dims)
    far, m, z = p.groups - 1, p.modes, p.planes
    field = f32(NB * p.pitch, LANES)
    return dict(
        f=f32(NODES, z, LANES),
        fo=f32(far, NI, z, LANES),
        spec=f32((NB + DEEP) * p.all_pitch, LANES),
        res=field,
        app=field,
        x=field,
        dir=field,
        along=field,
        cin=f32(NI, NB, m),
        sin=f32(NB, NB, m),
        iin=f32(NI, NI, m),
        cpack=f32(p.groups, p.couple_all, LANES),
        ipack=f32(p.groups, p.inner_all, LANES),
        cf=f32(p.all_modes * p.matrix, LANES),
        invf=f32(p.all_modes * TALL, LANES),
        sch=f32(m * p.matrix, LANES),
        cbuf=f32(NB * p.chunk_pitch, LANES),
        cgrid=f32(NB * p.chunk, LANES),
        sbuf=f32(far, p.chunks, PLANES * p.chunk, LANES),
        rbuf=f32(far, p.chunks, PLANES * p.chunk, LANES),
        xsend=f32(p.parts, PLANES * p.part, LANES),
        xr=f32(far, p.parts, PLANES * p.part, LANES),
        fwd=half(p.groups, p.all_modes, 3 * z),
        back=half(z, 3 * m),
        far=half(far * p.parts, z, 3 * p.part),
        one=half(LANES, LANES),
        oneT=half(LANES, LANES),
        scale=f32(8, LANES),
        coef=f32(1, LANES),
        cell=pltpu.VMEM((1, LANES), jnp.int32),
        keep=f32(NB, LANES),
        weight=f32(NB, LANES),
        xs=f32(ITERS, 2, 2, m, LANES),
        xh=f32(ITERS, 2, 2, m, LANES),
        ys=f32(ITERS, 2, m, LANES),
        yh=f32(ITERS, 3, 2, m, LANES),
        ps=f32(ITERS, p.peers, 1, 2 * m),
        pr=f32(ITERS, p.peers, 1, 2 * m),
        s_local=dma(7),
        s_halo=dma(2, ITERS, 8),
        s_sum=dma(2, ITERS),
        s_couple=dma(2, 1 + p.couple_bits, far, 1),
        s_inner=dma(2, 3, far, max(1, p.ex - 1, p.ey - 1)),
        s_f1=dma(2, far, p.chunks),
        s_f2=dma(2, far, 4),
        s_b1=dma(2, far, p.parts),
    )


def kernel(p, names, forcing, coef_in, cell_in, schur_in, couple_in, inner_in, table, out, *refs):
    s = types.SimpleNamespace(**dict(zip(names, refs)))
    m, z, gm, mc = p.modes, p.planes, p.all_modes, p.chunk
    mp, gp, cp, nb = p.pitch, p.all_pitch, p.chunk_pitch, p.matrix
    mo = p.part
    cells = LANES
    sizes = {"fourier": p.groups, "ex": p.ex, "ey": p.ey}
    place = {axis: lax.axis_index(axis) for axis in sizes}
    lane = lax.broadcasted_iota(jnp.int32, (m, cells), 1)
    lane_row = lane // ELY
    lane_col = lane % ELY

    def shifted(axis, by):
        return lax.rem(place[axis] + (by % sizes[axis]), sizes[axis])

    def remote(source, target, sems, index, device):
        return pltpu.make_async_remote_copy(
            src_ref=source,
            dst_ref=target,
            send_sem=sems.at[(0,) + index],
            recv_sem=sems.at[(1,) + index],
            device_id=device,
            device_id_type=pl.DeviceIdType.MESH,
        )

    hops = range(1, p.groups)
    around = [(a, b) for a in range(p.ex) for b in range(p.ey) if a or b]

    bottom = lambda k: k
    top = lambda k: 3 * P_SIZE - k
    left = lambda k: (NB - k) % NB
    right = lambda k: P_SIZE + k
    last = cells - ELY

    def turned(value, shift):
        shift = shift % cells
        return pltpu.roll(value, shift, 1) if shift else value

    def grid(rows):
        where = lax.broadcasted_iota(jnp.int32, (rows, cells), 1)
        return where // ELY, where % ELY

    def compress(load, store, rows):
        row, col = grid(rows)

        def sideways(k):
            return load(left(k)) + jnp.where(row == 0, 0.0, turned(load(right(k)), ELY))

        corner = sideways(P_SIZE)
        store(0, sideways(0) + jnp.where(col == 0, 0.0, turned(corner, 1)))
        for k in range(1, P_SIZE):
            store(k, load(k) + jnp.where(col == 0, 0.0, turned(load(top(k)), 1)))
            store(P_SIZE - 1 + k, sideways(k))
        edge = load(right(0)) + jnp.where(col == 0, 0.0, turned(load(right(P_SIZE)), 1))
        far_row = turned(edge, -last)
        far_col = turned(corner, 1 - ELY)
        for k in range(1, P_SIZE):
            far_row = jnp.where(row == k, turned(load(right(k)), ELY * k - last), far_row)
            far_col = jnp.where(col == k, turned(load(top(k)), k - ELY + 1), far_col)
        tip = turned(load(top(P_SIZE)), P_SIZE - ELY + 1)
        store(2 * P_SIZE - 1, far_row)
        store(
            2 * P_SIZE,
            jnp.where(
                col < P_SIZE,
                far_col,
                jnp.where((col == P_SIZE) & (row == ELX - 1), tip, 0.0),
            ),
        )

    def pick_planes(load, store, rows):
        row, col = grid(rows)
        far_row = turned(load(right(0)), -last)
        far_col = turned(load(top(0)), 1 - ELY)
        for k in range(P_SIZE):
            store(k, load(k))
        for k in range(1, P_SIZE):
            store(P_SIZE - 1 + k, load(left(k)))
            far_row = jnp.where(row == k, turned(load(right(k)), ELY * k - last), far_row)
        for k in range(1, P_SIZE + 1):
            far_col = jnp.where(col == k, turned(load(top(k)), k - ELY + 1), far_col)
        store(2 * P_SIZE - 1, far_row)
        store(2 * P_SIZE, far_col)

    def spread(load, n, rows, inside):
        row, col = grid(rows)
        if n < P_SIZE:
            return load(n)
        if n > 3 * P_SIZE:
            return load(P_SIZE - 1 + NB - n)
        if n < 2 * P_SIZE:
            k = n - P_SIZE
            beside = turned(load(k and P_SIZE - 1 + k), -ELY) if inside else 0.0
            return jnp.where(
                row == ELX - 1, turned(load(2 * P_SIZE - 1), last - ELY * k), beside
            )
        k = 3 * P_SIZE - n
        if inside:
            above = turned(load(k) if k < P_SIZE else spread(load, P_SIZE, rows, True), -1)
        else:
            above = 0.0
        return jnp.where(col == ELY - 1, turned(load(2 * P_SIZE), ELY - 1 - k), above)

    def planes_of(ref, rows):
        return lambda k: ref[k * rows : (k + 1) * rows, :]

    loads = [
        pltpu.make_async_copy(couple_in, s.cin, s.s_local.at[0]),
        pltpu.make_async_copy(inner_in, s.iin, s.s_local.at[1]),
        pltpu.make_async_copy(
            forcing.at[pl.ds(NB, NI)], s.f.at[pl.ds(NB, NI)], s.s_local.at[2]
        ),
        pltpu.make_async_copy(forcing.at[pl.ds(0, NB)], s.f.at[pl.ds(0, NB)], s.s_local.at[3]),
        pltpu.make_async_copy(schur_in, s.sin, s.s_local.at[4]),
        pltpu.make_async_copy(coef_in, s.coef, s.s_local.at[5]),
        pltpu.make_async_copy(cell_in, s.cell, s.s_local.at[6]),
    ]
    for k in (0, 2, 3, 5, 6, 1, 4):
        loads[k].start()

    s.xh[...] = jnp.zeros_like(s.xh)
    s.yh[...] = jnp.zeros_like(s.yh)

    barrier = pltpu.get_barrier_semaphore()
    for a, b in around:
        pl.semaphore_signal(
            barrier,
            inc=1,
            device_id={"ex": shifted("ex", a), "ey": shifted("ey", b)},
            device_id_type=pl.DeviceIdType.MESH,
        )
    for hop in hops:
        pl.semaphore_signal(
            barrier,
            inc=1,
            device_id={"fourier": shifted("fourier", hop)},
            device_id_type=pl.DeviceIdType.MESH,
        )

    def clear(ref, start, stop):
        if stop > start:
            ref[pl.ds(start, stop - start), :] = jnp.zeros((stop - start, LANES), jnp.float32)

    br = p.couple_rows
    own_rows = NI * br
    got_rows = p.couple_part * p.couple_ways
    clear(s.cpack.at[0], own_rows, got_rows)
    loads[0].wait()
    for i in range(NI):
        s.cpack[0, i * br : (i + 1) * br, :] = jnp.concatenate(
            [s.cin[i, k * br : (k + 1) * br, :] for k in range(p.fold)], 1
        )
    pl.semaphore_wait(barrier, len(around) + p.groups - 1)

    def share_by_halves(pack, part, sems):
        stages, bits = [], p.couple_bits
        digit = [place["ey"] // 2**k % 2 for k in range(bits)]
        turn = sum(digit[k] * 2 ** (bits - 1 - k) for k in range(bits))
        for stage in range(bits + 1):
            held = 2 ** max(0, stage - 1)
            rows = tile(turn // held * (held * part), held * part)
            if stage:
                flip = 2 ** (bits - stage)
                other = {"ey": place["ey"] + flip * (1 - 2 * digit[bits - stage])}
            stages.append(
                [
                    remote(
                        pack.at[g if stage else 0, rows], pack.at[g, rows], sems,
                        (stage, g - 1, 0),
                        other if stage else {"fourier": shifted("fourier", g)},
                    )
                    for g in hops
                ]
            )
        return stages

    def share_out(pack, part, sems):
        turn = place["ey"] * p.ex + place["ex"]
        rows = tile(turn * part, part)
        stages = [
            [
                remote(
                    pack.at[0, rows], pack.at[g, rows], sems, (0, g - 1, 0),
                    {"fourier": shifted("fourier", g)},
                )
                for g in hops
            ]
        ]
        for axis in ("ex", "ey"):
            if axis == "ey":
                rows = tile(place["ey"] * p.ex * part, p.ex * part)
            stages.append(
                [
                    remote(
                        pack.at[g, rows], pack.at[g, rows], sems, (len(stages), g - 1, k - 1),
                        {axis: shifted(axis, k)},
                    )
                    for g in hops
                    for k in range(1, sizes[axis])
                ]
            )
        return stages

    def start(stage):
        for copy in stage:
            copy.start()

    def arrive(stage):
        for copy in stage:
            copy.wait_recv()

    couple = share_by_halves(s.cpack, p.couple_part, s.s_couple)
    inner_parts = share_out(s.ipack, p.inner_part, s.s_inner)
    start(couple[0])

    bounds = [0, 8, 22, 36, NI]
    second = [
        [
            remote(
                s.f.at[pl.ds(NB + a, b - a)], s.fo.at[g - 1, pl.ds(a, b - a)], s.s_f2,
                (g - 1, k), {"fourier": shifted("fourier", g)},
            )
            for g in hops
        ]
        for k, (a, b) in enumerate(zip(bounds, bounds[1:]))
    ]
    loads[2].wait()
    start(second[0])

    clear(s.cpack.at[0], got_rows, p.couple_all)
    for g in hops:
        clear(s.cpack.at[g], got_rows, p.couple_all)

    for g in range(p.groups):
        s.fwd[g] = stacked(table[:, g * z : (g + 1) * z])

    def flat(pack, g, start, count, stride, width):
        rows = pack[g, pl.ds(start, count, stride=stride) if stride > 1 else pl.ds(start, count), :]
        if count < LANES:
            rows = jnp.concatenate([rows, jnp.zeros((LANES - count, LANES), jnp.float32)], 0)
        return jnp.transpose(rows)

    def couple_matrices(g):
        for b in range(br):
            turned_rows = flat(s.cpack, g, b, DEEP, br, NI)
            for k in range(p.fold):
                s.cf[pl.ds(g * m * nb + k * br + b, m, stride=nb), :] = turned_rows[
                    k * m : (k + 1) * m
                ]

    def inner_matrices(g):
        for i in range(ir):
            turned_rows = flat(s.ipack, g, i * TALL, TALL, 1, NI)
            for k in range(p.fold):
                if k * ir + i < TALL:
                    s.invf[pl.ds(g * m * TALL + k * ir + i, m, stride=TALL), :] = turned_rows[
                        k * m : (k + 1) * m
                    ]

    def spectrum(nodes):
        values = apply_table(s.fwd[0], [s.f[n] for n in nodes])
        for n, value in zip(nodes, values):
            s.spec[tile(n * gp, gm), :] = value

    clear(s.spec, NODES * gp, (NB + DEEP) * gp)
    pairs(NB, NODES, 4, spectrum)
    loads[3].wait()
    pairs(0, NB, 4, spectrum)
    couple_matrices(0)

    loads[5].wait()
    loads[6].wait()
    lines = lax.broadcasted_iota(jnp.int32, (LANES, LANES), 0)
    hot = jnp.where(lines == s.cell[...], 1.0, 0.0).astype(jnp.float32)
    hot_t = jnp.transpose(hot)
    s.oneT[...] = hot.astype(jnp.bfloat16)
    s.one[...] = hot_t.astype(jnp.bfloat16)
    s.scale[...] = lax.dot_general(
        jnp.broadcast_to(s.coef[...], (8, LANES)),
        hot_t,
        (((1,), (0,)), ((), ())),
        precision=HIGHEST,
        preferred_element_type=jnp.float32,
    )

    def permuted(rows, hot_ref):
        both = dot(jnp.concatenate(split(rows), 0), hot_ref[...])
        return both[: rows.shape[0]] + both[rows.shape[0] :]

    def condense(g, c, store):
        def one_mode(k):
            j = g * m + c * mc + k
            inner = s.spec[pl.ds(NB * gp + j, DEEP, stride=gp), :]
            matrix = s.cf[tile(j * nb, NB), :DEEP]
            s.cbuf[pl.ds(k, NB, stride=cp), :] = s.spec[
                pl.ds(j, NB, stride=gp), :
            ] - product(matrix, inner)

        loop(mc, 16, one_mode)
        per = WIDE // mc
        for block in range(NB // per):
            rows = [s.cbuf[n * cp : n * cp + mc, :] for n in range(block * per, (block + 1) * per)]
            store(block, permuted(jnp.concatenate(rows, 0), s.one))

    def keep_own(c):
        per = WIDE // mc

        def store(block, rows):
            for k in range(per):
                n = block * per + k
                s.res[n * mp + c * mc : n * mp + (c + 1) * mc, :] = rows[k * mc : (k + 1) * mc]

        return store

    own_chunks = list(range(p.chunks))

    def condense_own():
        if own_chunks:
            c = own_chunks.pop(0)
            condense(0, c, keep_own(c))

    arrive(couple[0])
    for copies in couple[1:2]:
        start(copies)
    condense_own()
    loads[1].wait()
    ir = p.inner_rows
    clear(s.ipack.at[0], 0, p.inner_all)
    for i in range(ir):
        picks = [s.iin[min(k * ir + i, NI - 1), :, :] for k in range(p.fold)]
        s.ipack[0, i * TALL : i * TALL + NI, :] = jnp.concatenate(picks, 1)
    start(inner_parts[0])

    for stage, copies in enumerate(couple[2:]):
        if stage == 0:
            condense_own()
        arrive(couple[stage + 1])
        start(copies)
    condense_own()
    arrive(inner_parts[0])
    start(inner_parts[1])
    arrive(couple[-1])

    first = []
    for g in hops:
        couple_matrices(g)
        for c in range(p.chunks):

            def store(block, rows):
                s.cgrid[block * WIDE : (block + 1) * WIDE, :] = rows

            condense(g, c, store)

            def put(k, value, g=g, c=c):
                s.sbuf[g - 1, c, k * mc : (k + 1) * mc, :] = value

            compress(planes_of(s.cgrid, mc), put, mc)
            copy = remote(
                s.sbuf.at[g - 1, c], s.rbuf.at[g - 1, c], s.s_f1, (g - 1, c),
                {"fourier": shifted("fourier", -g)},
            )
            copy.start()
            first.append((g, c, copy))

    for stage in second[1:]:
        start(stage)
    arrive(inner_parts[1])
    start(inner_parts[2])

    while own_chunks:
        condense_own()

    flipped = jnp.transpose(table[...])[:z]
    s.back[...] = stacked(flipped[:, :m])
    for k in range((p.groups - 1) * p.parts):
        s.far[k] = stacked(flipped[:, m + k * mo : m + (k + 1) * mo])

    loads[4].wait()
    group = LANES // NB
    for q in range(NB // group):
        rows = jnp.concatenate([s.sin[q * group + k] for k in range(group)], 0)
        if m < LANES:
            rows = jnp.concatenate([rows, jnp.zeros((LANES, LANES - m), jnp.float32)], 1)
        square = jnp.transpose(rows)[:m]
        high = square.astype(jnp.bfloat16).astype(jnp.float32)
        low = square - high
        where = lax.broadcasted_iota(jnp.int32, (m, LANES), 1)
        for k in range(group):
            first_half = jnp.where(where < NB, turned(high, -k * NB), turned(high, NB - k * NB))
            s.sch[pl.ds(q * group + k, m, stride=nb), :] = jnp.where(
                where < 2 * NB, first_half, turned(low, 2 * NB - k * NB)
            )

    slots = lax.broadcasted_iota(jnp.int32, (NB, cells), 0)
    places = lax.broadcasted_iota(jnp.int32, (NB, cells), 1)
    row_ids = place["ex"] * ELX + places // ELY
    col_ids = place["ey"] * ELY + places % ELY
    dropped = (
        ((slots == 0) | (slots >= 3 * P_SIZE)) & (row_ids == 0)
        | (slots >= P_SIZE) & (slots <= 2 * P_SIZE) & (row_ids == ELX * p.ex - 1)
        | (slots <= P_SIZE) & (col_ids == 0)
        | (slots >= 2 * P_SIZE) & (slots <= 3 * P_SIZE) & (col_ids == ELY * p.ey - 1)
    )
    keep = jnp.where(dropped, 0.0, 1.0).astype(jnp.float32)
    s.keep[...] = keep
    s.weight[...] = keep * jnp.where(slots % P_SIZE == 0, 0.25, 0.5)

    def couple_beside(q):
        group = LANES // NB
        rows = [s.cf[tile((q * group + k) * nb, NB), :] for k in range(group)]
        square = jnp.transpose(jnp.concatenate(rows, 0))[:TALL]
        where = lax.broadcasted_iota(jnp.int32, (TALL, LANES), 1)
        for k in range(group):
            place_rows = tile((q * group + k) * TALL, TALL)
            s.invf[place_rows, :] = jnp.where(
                (where >= DEEP) & (where < DEEP + NB),
                -turned(square, DEEP - k * NB),
                s.invf[place_rows, :],
            )

    inner_matrices(0)

    def far_matrices():
        arrive(inner_parts[2])
        for g in hops:
            inner_matrices(g)

    fillers = [far_matrices, lambda: loop(gm * NB // LANES, 4, couple_beside)]

    def node(n):
        return tile(n * mp, m)

    def exists(axis, step):
        if step == 0:
            return None
        return place[axis] < sizes[axis] - 1 if step > 0 else place[axis] > 0

    def guarded(ex_step, ey_step, action):
        tests = [t for t in (exists("ex", ex_step), exists("ey", ey_step)) if t is not None]
        pl.when(functools.reduce(jnp.logical_and, tests))(action)

    def halo_copy(turn, number, source, target, ex_step, ey_step):
        copy = pltpu.make_async_remote_copy(
            src_ref=source,
            dst_ref=target,
            send_sem=s.s_halo.at[0, turn, number],
            recv_sem=s.s_halo.at[1, turn, number],
            device_id={"ex": shifted("ex", ex_step), "ey": shifted("ey", ey_step)},
            device_id_type=pl.DeviceIdType.MESH,
        )
        guarded(ex_step, ey_step, copy.start)
        return (
            lambda: guarded(-ex_step, -ey_step, copy.wait_recv),
            lambda: guarded(ex_step, ey_step, copy.wait_send),
        )

    def assemble(ref, turn, meanwhile):
        copies = []
        up = down = None
        for k in range(P_SIZE + 1):
            ends = jnp.where(lane_col == ELY - 1, ref[node(top(k)), :], ref[node(bottom(k)), :])
            ends = turned(ends, k)
            up = ends if k == 0 else jnp.where(lane_col == k - 1, ends, up)
            down = ends if k == 0 else jnp.where(lane_col == k, ends, down)
        up = jnp.where(lane_col <= P_SIZE, turned(up, 1 - ELY), 0.0)
        down = jnp.where(lane_col <= P_SIZE, down, 0.0)
        s.ys[turn, 0] = up
        s.ys[turn, 1] = down
        for slot, ex_step in ((1, 1), (2, -1), (0, 0)):
            for way, ey_step in ((0, 1), (1, -1)):
                copies.append(
                    halo_copy(
                        turn, 2 * slot + way, s.ys.at[turn, way], s.yh.at[turn, slot, way],
                        ex_step, ey_step,
                    )
                )
        for k in range(P_SIZE):
            ends = jnp.where(lane_row == ELX - 1, ref[node(right(k)), :], ref[node(left(k)), :])
            ends = turned(ends, ELY * k)
            up = ends if k == 0 else jnp.where(lane_row == k - 1, ends, up)
            down = ends if k == 0 else jnp.where(lane_row == k, ends, down)
        up = turned(up, -last)
        s.xs[turn, 0, 0] = up
        s.xs[turn, 1, 0] = down
        s.xs[turn, 0, 1] = turned(ref[node(right(P_SIZE)), :], -last)
        s.xs[turn, 1, 1] = ref[node(left(P_SIZE)), :]
        for way, ex_step in ((0, 1), (1, -1)):
            copies.append(
                halo_copy(turn, 6 + way, s.xs.at[turn, way], s.xh.at[turn, way], ex_step, 0)
            )

        for k in range(P_SIZE + 1):
            here_left, here_right = ref[node(left(k)), :], ref[node(right(k)), :]
            ref[node(left(k)), :] = here_left + jnp.where(
                lane_row == 0, 0.0, turned(here_right, ELY)
            )
            ref[node(right(k)), :] = here_right + jnp.where(
                lane_row == ELX - 1, 0.0, turned(here_left, -ELY)
            )
        meanwhile()
        for wait, _ in copies:
            wait()

        for k in range(P_SIZE + 1):
            part, lanes = divmod(k, P_SIZE)
            if part:
                low = s.xh[turn, 0, part]
                high = turned(s.xh[turn, 1, part], last)
            else:
                if k == 0:
                    from_low, from_high = s.xh[turn, 0, 0], turned(s.xh[turn, 1, 0], last)
                low = turned(jnp.where(lane_row == k, from_low, from_high), -ELY * k)
                high = low
            for n, halo, row in ((left(k), low, 0), (right(k), high, ELX - 1)):
                value = ref[node(n), :] + jnp.where(lane_row == row, halo, 0.0)
                if n % (2 * P_SIZE) > P_SIZE:
                    value = value * s.keep[n : n + 1, :]
                ref[node(n), :] = value

        lines = []
        for way in range(2):
            line = s.yh[turn, 0, way]
            before = jnp.where(
                lane == 0, turned(s.yh[turn, 1, way], P_SIZE), turned(line, P_SIZE)
            )
            after = jnp.where(
                lane == last + P_SIZE, turned(s.yh[turn, 2, way], -P_SIZE), turned(line, -P_SIZE)
            )
            lines.append(
                line
                + jnp.where(lane_col == 0, before, jnp.where(lane_col == P_SIZE, after, 0.0))
            )
        low_all, high_all = lines[0], turned(lines[1], ELY - 1)
        for k in range(P_SIZE + 1):
            b, t = bottom(k), top(k)
            here_bottom, here_top = ref[node(b), :], ref[node(t), :]
            ends = turned(jnp.where(lane_col == k, low_all, high_all), -k)
            ref[node(b), :] = s.keep[b : b + 1, :] * (
                here_bottom + jnp.where(lane_col == 0, ends, turned(here_top, 1))
            )
            ref[node(t), :] = s.keep[t : t + 1, :] * (
                here_top + jnp.where(lane_col == ELY - 1, ends, turned(here_bottom, -1))
            )
        for _, leave in copies:
            leave()

    def operator():
        scale = s.scale[0:1, :]

        def one_mode(k):
            value = s.res[pl.ds(k, NB, stride=mp), :]
            matrix = s.sch[tile(k * nb, NB), : 3 * NB].astype(jnp.bfloat16)
            s.app[pl.ds(k, NB, stride=mp), :] = dot(matrix, pile(value)) * scale

        loop(m, 8, one_mode)

    def sums_start(turn):
        def step(outer, sums):
            norm, curve = sums
            for inner in range(4):
                n = outer * 4 + inner
                mine = s.res[node(n), :]
                norm = norm + s.weight[pl.ds(n, 1), :] * mine * mine
                curve = curve + mine * s.app[node(n), :]
            return norm, curve

        zero = jnp.zeros((m, cells), jnp.float32)
        norm, curve = lax.fori_loop(0, NB // 4, step, (zero, zero))
        total = lax.dot_general(
            jnp.ones((8, cells), jnp.float32),
            jnp.concatenate([norm, curve], 0),
            (((1,), (1,)), ((), ())),
            precision=HIGHEST,
            preferred_element_type=jnp.float32,
        )
        for k in range(p.peers):
            s.ps[turn, k] = total[0:1, :]
        copies = [
            remote(
                s.ps.at[turn, k], s.pr.at[turn, k], s.s_sum, (turn,),
                {"ex": shifted("ex", a), "ey": shifted("ey", b)},
            )
            for k, (a, b) in enumerate(around)
        ]
        for copy in copies:
            copy.start()
        return copies

    def sums_end(turn, copies):
        whole = remote(
            s.ps.at[turn], s.pr.at[turn], s.s_sum, (turn,),
            {"ex": shifted("ex", around[0][0]), "ey": shifted("ey", around[0][1])},
        )
        whole.wait_recv()
        total = s.ps[turn, 0]
        for k in range(p.peers):
            total = total + s.pr[turn, k]
        whole.wait_send()
        row = lax.broadcasted_iota(jnp.int32, (m, 2 * m), 0)
        column = lax.broadcasted_iota(jnp.int32, (m, 2 * m), 1)
        pick = lambda offset: jnp.sum(
            jnp.where(column == row + offset, total, 0.0), axis=1, keepdims=True
        )
        return pick(0), pick(m)

    for g, c, copy in first:
        copy.wait_recv()

        arrived = planes_of(s.rbuf.at[g - 1, c], mc)
        for n in range(NB):
            rows = pl.ds(n * mp + c * mc, mc)
            s.res[rows, :] = s.res[rows, :] + spread(arrived, n, mc, False)

    def add_far(piece):
        def some_nodes(nodes):
            totals = [s.spec[tile((NB + n) * gp, gm), :] for n in nodes]
            for g in hops:
                more = apply_table(s.fwd[g], [s.fo[g - 1, n] for n in nodes])
                totals = [total + value for total, value in zip(totals, more)]
            for n, total in zip(nodes, totals):
                s.spec[tile((NB + n) * gp, gm), :] = total

        arrive(second[piece])
        pairs(bounds[piece], bounds[piece + 1], 4, some_nodes)

    assemble(s.res, 0, lambda: add_far(0))

    carry = None
    for turn in range(ITERS):
        operator()
        copies = sums_start(turn)
        if turn < ITERS - 1:
            assemble(s.app, turn + 1, fillers[turn])
        else:
            add_far(1)
        norm, curve = sums_end(turn, copies)
        if turn == 0:
            step_size = norm / curve
        else:
            ratio = norm / carry[0]
            step_size = norm / (curve - ratio * norm / carry[1])
        carry = norm, step_size

        def update(n, turn=turn):
            rows = node(n)
            search, along = s.res[rows, :], s.app[rows, :]
            residual = search
            if turn:
                search = search + ratio * s.dir[rows, :]
                s.x[rows, :] = s.x[rows, :] + step_size * search
            else:
                s.x[rows, :] = step_size * search
            if turn < ITERS - 1:
                if turn:
                    along = along + ratio * s.along[rows, :]
                s.dir[rows, :] = search
                s.along[rows, :] = along
                s.res[rows, :] = residual - step_size * along

        loop(NB, 4, update)

    def solved(c):
        return lambda n: s.x[n * mp + c * mo : n * mp + (c + 1) * mo, :]

    third = []
    for c in range(p.parts):

        def put(k, value, c=c):
            s.xsend[c, k * mo : (k + 1) * mo, :] = value

        pick_planes(solved(c), put, mo)
        for g in hops:
            copy = remote(
                s.xsend.at[c], s.xr.at[g - 1, c], s.s_b1, (g - 1, c),
                {"fourier": shifted("fourier", g)},
            )
            copy.start()
            third.append((g, c, copy))

    for copies in couple + inner_parts + second:
        for copy in copies:
            copy.wait_send()
    for _, _, copy in first:
        copy.wait_send()

    for piece in range(2, len(second)):
        add_far(piece)
    inverse_coef = 1.0 / s.coef[...]

    def restore(g, c, load):
        per = WIDE // mo
        for block in range(NB // per):
            nodes = range(block * per, (block + 1) * per)
            rows = permuted(jnp.concatenate([load(n) for n in nodes], 0), s.oneT)
            for k, n in enumerate(nodes):
                start_row = n * gp + g * m + c * mo
                s.spec[start_row : start_row + mo, :] = rows[k * mo : (k + 1) * mo]

    def inner_rows(j, count):
        return pl.ds(NB * gp + j, count, stride=gp)

    def matrix(j, lanes):
        return s.invf[tile(j * TALL, TALL), lanes]

    def scaled(j):
        return s.spec[inner_rows(j, DEEP), :] * inverse_coef

    def cycle(j):
        return s.spec[pl.ds(j, NB, stride=gp), :]

    def whole_mode(j):
        both = jnp.concatenate([scaled(j), cycle(j)], 0)
        s.spec[inner_rows(j, NI), :] = product(matrix(j, pl.ds(0, DEEP + NB)), both)[:NI]

    def base(j):
        s.spec[inner_rows(j, NI), :] = product(matrix(j, pl.ds(0, DEEP)), scaled(j))[:NI]

    def correct(j):
        value = product(matrix(j, pl.ds(DEEP, NB)), cycle(j))
        s.spec[inner_rows(j, NI), :] = s.spec[inner_rows(j, NI), :] + value[:NI]

    for c in range(p.parts):
        restore(0, c, solved(c))
        loop(mo, 16, lambda k, c=c: whole_mode(c * mo + k))

    def own_velocity(nodes):
        rows = [s.spec[tile(n * gp, m), :] for n in nodes]
        for n, value in zip(nodes, apply_table(s.back[...], rows)):
            out[n] = value

    pairs(0, NODES, 4, own_velocity)

    late = gm - mo
    loop(mo, 16, lambda k: base(late + k))

    for g, c, copy in third:
        copy.wait_recv()
        arrived = planes_of(s.xr.at[g - 1, c], mo)
        restore(g, c, lambda n, arrived=arrived: spread(arrived, n, mo, True))
        first_mode = g * m + c * mo

        def far_mode(k, first_mode=first_mode):
            if first_mode == late:
                correct(first_mode + k)
            else:
                whole_mode(first_mode + k)

        loop(mo, 16, far_mode)

        def far_velocity(nodes, g=g, c=c, first_mode=first_mode):
            rows = [s.spec[tile(n * gp + first_mode, mo), :] for n in nodes]
            values = apply_table(s.far[(g - 1) * p.parts + c], rows)
            for n, value in zip(nodes, values):
                out[n] = out[n] + value

        pairs(0, NODES, 4, far_velocity)

    for _, _, copy in third:
        copy.wait_send()


def on_device(forcing, element_coef, schur, couple, inner_inv, element_cell):
    planes, _, elements = forcing.shape
    modes = schur.shape[0]
    sizes = tuple(lax.axis_size(axis) for axis in ("fourier", "ex", "ey"))
    p = Plan(sizes, modes, planes)
    me = lax.axis_index("fourier")
    length = planes * p.groups

    def ordered(dim, size):
        place = lax.broadcasted_iota(jnp.int32, (length, length), dim)
        return lax.rem(me + p.groups - place // size, p.groups) * size + place % size

    table = dft_values(ordered(0, modes), ordered(1, planes), length)
    pinned = lambda value: pltpu.with_memory_space_constraint(value, pltpu.HBM)
    scratch = layout(p)
    whole = pl.BlockSpec(memory_space=pltpu.VMEM)
    stay = pl.BlockSpec(memory_space=pltpu.HBM)
    velocity = pl.pallas_call(
        functools.partial(kernel, p, tuple(scratch)),
        out_shape=jax.ShapeDtypeStruct((NODES, planes, elements), jnp.float32),
        in_specs=[stay] * 6 + [whole],
        out_specs=whole,
        scratch_shapes=list(scratch.values()),
        compiler_params=pltpu.CompilerParams(
            collective_id=0, has_side_effects=True, vmem_limit_bytes=44 << 20
        ),
        cost_estimate=pl.CostEstimate(flops=10**9, bytes_accessed=2 * 10**8, transcendentals=0),
    )(
        pinned(jnp.transpose(forcing, (1, 0, 2))),
        pinned(element_coef[None]),
        pinned(element_cell[None]),
        pinned(jnp.transpose(schur, (1, 2, 0))),
        pinned(jnp.transpose(couple, (2, 1, 0))),
        pinned(jnp.transpose(inner_inv, (1, 2, 0))),
        table,
    )
    return jnp.transpose(velocity, (1, 0, 2))


def solution(mesh):
    placed = (
        P("fourier", None, ("ex", "ey")),
        P(("ex", "ey")),
        P("fourier", None, None),
        P("fourier", None, None),
        P("fourier", None, None),
        P(("ex", "ey")),
    )
    return jax.shard_map(
        on_device,
        mesh=mesh,
        in_specs=placed,
        out_specs=P("fourier", None, ("ex", "ey")),
        check_vma=False,
    )
```
